1024 devices in a mesh: dom: 64 (over x, z), sub: 16 (over y, core).
Axes of the slice: x: 8, y: 8, z: 8, core: 2. Of those that a mesh axis runs over, the one named last changes fastest.
Arguments:
- load_vector: float32 [2048, 128], P(('dom', 'sub')), may hold values from -38 to 38
- recycled: float32 [40, 2048, 128], P(None, ('dom', 'sub')), may hold values from -80 to 80
- images: float32 [40, 2048, 128], P(None, ('dom', 'sub')), may hold values from -6 to 6
- matrix_tiles: float32 [2048, 8, 128, 128], P(('dom', 'sub')), may hold values from -7 to 7
- tile_columns: int32 [2048, 8], P(('dom', 'sub')), may hold values from 0 to 5, as said below
- ghost_list: int32 [1024, 4], P(('dom', 'sub')), may hold values from 0 to 95, as said below
- live_counts: int32 [1024], P(('dom', 'sub')), may hold values from 1 to 2, as said below
Outputs:
- solution: float32 [2048, 128], P(('dom', 'sub'))
- residual: float32 [2048, 128], P(('dom', 'sub'))
The draws below stay inside these ranges and needn't reach their ends.
Inputs may be any that keep to these rules, and one draw needn't show every extreme that they name: `live_counts`: each device's live block rows are its first slots; some device has all 2 live. `tile_columns`: tile 0 of a block row names the row's own slot. Other entries below 2 name a live slot of the same device; entries from 2 on name a ghost slot of that device. `ghost_list`: each entry names a live slot q of a device with sub index s and dom index differing from the owner's by o - 1 (o of 0, 1, 2), coded as o * (size of sub) * 2 + s * 2 + q; it never points outside the dom axis and never to the owner itself.
All inputs are finite; a program needn't handle non-finite values.
Results may differ from the reference program's by a relative error of at most 0.0003.
Values sent between devices are 32-bit elements; how exact they have to be, the bound alone decides.
A program may use at most 32 MiB of HBM per device.

```python
import math
import jax
import jax.numpy as jnp
from jax import lax

SLOTS = 2
BLK = 128
TPR = 8
K = 40
STEPS = 3
GHOSTS = 4
ROWBLOCKS = 2048
ROWS = 262144
N_DOM = 64
N_SUB = 16
DEVICES = 1024


def live_draw(key):
    base = jax.random.fold_in(key, 101)
    first_key, second_key, third_key = jax.random.split(base, 3)
    factor_a = jax.random.randint(first_key, (DEVICES,), 0, SLOTS + 1)
    factor_b = jax.random.randint(second_key, (DEVICES,), 0, SLOTS + 1)
    counts = 1 + jnp.minimum(factor_a * factor_b // SLOTS, SLOTS - 1)
    chosen = jax.random.randint(third_key, (), 0, DEVICES)
    counts = jnp.where(jnp.arange(DEVICES) == chosen, SLOTS, counts)
    return counts.astype(jnp.int32)


def draw_live_counts(key, part):
    return live_draw(key)


def draw_ghost_list(key, part):
    counts = live_draw(key)
    base = jax.random.fold_in(key, 202)
    first_key, second_key, third_key = jax.random.split(base, 3)
    device = jnp.arange(DEVICES, dtype=jnp.int32)[:, None]
    dom_index = device // N_SUB
    sub_index = device % N_SUB
    offset = jax.random.randint(first_key, (DEVICES, GHOSTS), 0, 3) - 1
    offset = jnp.where(dom_index + offset < 0, 1, offset)
    offset = jnp.where(dom_index + offset >= N_DOM, -1, offset)
    peer = jax.random.randint(second_key, (DEVICES, GHOSTS), 0, N_SUB)
    peer = jnp.where((offset == 0) & (peer == sub_index), (peer + 1) % N_SUB, peer)
    neighbour = (dom_index + offset) * N_SUB + peer
    slot_pick = jax.random.randint(third_key, (DEVICES, GHOSTS), 0, 1 << 20) % counts[neighbour]
    return ((offset + 1) * N_SUB * SLOTS + peer * SLOTS + slot_pick).astype(jnp.int32)


def draw_tile_columns(key, part):
    counts = live_draw(key)
    base = jax.random.fold_in(key, 303)
    first_key, second_key, third_key = jax.random.split(base, 3)
    block_row = jnp.arange(ROWBLOCKS, dtype=jnp.int32)
    device = block_row // SLOTS
    own_slot = block_row % SLOTS
    coin_flip = jax.random.randint(first_key, (ROWBLOCKS, TPR), 0, 2)
    local_pick = jax.random.randint(second_key, (ROWBLOCKS, TPR), 0, 1 << 20) % counts[device][:, None]
    ghost_pick = SLOTS + jax.random.randint(third_key, (ROWBLOCKS, TPR), 0, GHOSTS)
    columns = jnp.where(coin_flip == 1, ghost_pick, local_pick)
    columns = jnp.where(jnp.arange(TPR)[None, :] == 0, own_slot[:, None], columns)
    return columns.astype(jnp.int32)


def draw_matrix_tiles(key, part):
    base = jax.random.fold_in(key, 404)
    first_key, second_key = jax.random.split(base, 2)
    shape = (ROWBLOCKS, TPR, BLK, BLK)
    noise = jnp.clip(jax.random.normal(first_key, shape, jnp.float32), -5.0, 5.0)
    diagonal = jax.random.uniform(second_key, (ROWBLOCKS, 1, BLK, 1), jnp.float32, 2.0, 6.0)
    tile_index = jnp.arange(TPR)[None, :, None, None]
    scale = jnp.where(tile_index == 0, 0.5 / math.sqrt(BLK), 1.0 / math.sqrt(BLK * TPR))
    identity = jnp.eye(BLK, dtype=jnp.float32)[None, None]
    first_tile = jnp.where(tile_index == 0, 1.0, 0.0)
    return (noise * scale + first_tile * identity * diagonal).astype(jnp.float32)


def draw_load_vector(key, part):
    base = jax.random.fold_in(key, 505)
    first_key, second_key = jax.random.split(base, 2)
    device = (jnp.arange(ROWBLOCKS) // SLOTS).astype(jnp.float32)
    trend = 1.0 + 2.0 * device / (DEVICES - 1)
    spread = jnp.power(10.0, jax.random.uniform(second_key, (ROWBLOCKS, BLK), jnp.float32, 0.0, 1.0))
    values = jnp.clip(jax.random.normal(first_key, (ROWBLOCKS, BLK), jnp.float32), -5.0, 5.0)
    return (values * trend[:, None] * spread / 4.0).astype(jnp.float32)


def block_scale(key, extent, shards, low, largest):
    gain, own = 1.0, jax.random.fold_in(key, 6)
    for position, blocks in shards:
        heights = jnp.exp(jax.random.uniform(jax.random.fold_in(own, position), (blocks,), jnp.float32, low / len(shards), largest / len(shards)))
        gain = gain * jnp.repeat(heights, extent[position] // blocks).reshape([-1 if axis == position else 1 for axis in range(len(extent))])
    return gain


def bell_draw(own_key, extent, scale, bound, cuts=(), kind=jnp.bfloat16):
    level = block_scale(own_key, extent, cuts, -0.22, 0.18) if cuts else 1.0
    entries = jax.random.normal(own_key, extent, jnp.float32) * scale * level
    return jnp.minimum(jnp.maximum(entries, -bound), bound).astype(kind)


def setup_inputs(seed: int = 0) -> dict:
    seeds = jax.random.split(jax.random.key(seed), 8)
    return {
        "load_vector": draw_load_vector(jax.random.fold_in(seeds[7], 71), 0),
        "recycled": bell_draw(seeds[1], (K, ROWBLOCKS, BLK), (ROWS ** 0.5 / K), 80.0, ((1, 1024),), jnp.float32),
        "images": bell_draw(seeds[2], (K, ROWBLOCKS, BLK), 1.0, 6.0, ((1, 1024),), jnp.float32),
        "matrix_tiles": draw_matrix_tiles(jax.random.fold_in(seeds[7], 71), 0),
        "tile_columns": draw_tile_columns(jax.random.fold_in(seeds[7], 71), 0),
        "ghost_list": draw_ghost_list(jax.random.fold_in(seeds[7], 71), 0),
        "live_counts": draw_live_counts(jax.random.fold_in(seeds[7], 71), 0),
    }


def triangle_solve(factor, values, transpose):
    column = values if values.ndim == 2 else values[:, None]
    solved = lax.linalg.triangular_solve(factor, column, left_side=True, lower=True, transpose_a=transpose)
    return solved if values.ndim == 2 else solved[:, 0]

def global_columns(tile_columns, ghost_list):
    block_row = jnp.arange(ROWBLOCKS, dtype=jnp.int32)
    device = block_row // SLOTS
    ghost_rows = ghost_list[device]
    ghost_slot = jnp.clip(tile_columns - SLOTS, 0, GHOSTS - 1).astype(jnp.int32)
    ghost_code = jnp.take_along_axis(ghost_rows, ghost_slot, axis=1)
    group_size = N_SUB * SLOTS
    offset = ghost_code // group_size
    remainder = ghost_code % group_size
    dom_index = (device // N_SUB)[:, None]
    remote = ((dom_index + offset - 1) * N_SUB + remainder // SLOTS) * SLOTS + remainder % SLOTS
    local = device[:, None] * SLOTS + tile_columns
    return jnp.where(tile_columns < SLOTS, local, remote).astype(jnp.int32)

def apply_matrix(vector, matrix_tiles, columns, live_mask):
    picked = vector.reshape(ROWBLOCKS, BLK)[columns]
    product = jnp.einsum('rtij,rtj->ri', matrix_tiles, picked, precision=lax.Precision.HIGHEST)
    return (product * live_mask).reshape(-1)

def reference(load_vector, recycled, images, matrix_tiles, tile_columns, ghost_list, live_counts):
    highest = lax.Precision.HIGHEST
    block_row = jnp.arange(ROWBLOCKS, dtype=jnp.int32)
    live_mask = (block_row % SLOTS < live_counts[block_row // SLOTS]).astype(jnp.float32)[:, None]
    columns = global_columns(tile_columns, ghost_list)
    source = (load_vector * live_mask).reshape(-1)
    recycled_flat = (recycled * live_mask[None]).reshape(K, -1)
    images_flat = (images * live_mask[None]).reshape(K, -1)
    gram_matrix = jnp.dot(images_flat, images_flat.T, precision=highest)
    projection = jnp.dot(images_flat, source, precision=highest)
    source_norm = jnp.sum(source * source)
    cholesky_low = jnp.linalg.cholesky(gram_matrix)
    reduced = triangle_solve(cholesky_low, projection, False)
    start_coef = triangle_solve(cholesky_low, reduced, True)
    initial_norm = jnp.sqrt(source_norm - jnp.sum(reduced * reduced))
    start_point = jnp.dot(start_coef, recycled_flat, precision=highest)
    start_residual = source - jnp.dot(start_coef, images_flat, precision=highest)
    basis = [start_residual / initial_norm]
    hessenberg = jnp.zeros((STEPS + 1, STEPS), jnp.float32)
    coupling = jnp.zeros((K, STEPS), jnp.float32)
    for column in range(STEPS):
        image_now = apply_matrix(basis[column], matrix_tiles, columns, live_mask)
        stacked = jnp.stack(basis)
        against_images = triangle_solve(cholesky_low, jnp.dot(images_flat, image_now, precision=highest), False)
        against_basis = jnp.dot(stacked, image_now, precision=highest)
        image_norm = jnp.sum(image_now * image_now)
        next_norm = jnp.sqrt(image_norm - jnp.sum(against_images * against_images) - jnp.sum(against_basis * against_basis))
        back_coef = triangle_solve(cholesky_low, against_images, True)
        remaining = image_now - jnp.dot(back_coef, images_flat, precision=highest) - jnp.dot(against_basis, stacked, precision=highest)
        basis.append(remaining / next_norm)
        hessenberg = hessenberg.at[:column + 1, column].set(against_basis)
        hessenberg = hessenberg.at[column + 1, column].set(next_norm)
        coupling = coupling.at[:, column].set(against_images)
    normal_matrix = jnp.dot(hessenberg.T, hessenberg, precision=highest)
    target = initial_norm * hessenberg[0]
    small_factor = jnp.linalg.cholesky(normal_matrix)
    least = triangle_solve(small_factor, triangle_solve(small_factor, target, False), True)
    every_basis = jnp.stack(basis)
    update_coef = triangle_solve(cholesky_low, jnp.dot(coupling, least, precision=highest), True)
    solution = start_point + jnp.dot(least, every_basis[:STEPS], precision=highest) - jnp.dot(update_coef, recycled_flat, precision=highest)
    residual = start_residual - jnp.dot(jnp.dot(hessenberg, least, precision=highest), every_basis, precision=highest)
    return (solution.reshape(ROWBLOCKS, BLK), residual.reshape(ROWBLOCKS, BLK))
```

```python
import functools

import jax
import jax.numpy as jnp
from jax import lax
from jax.experimental import pallas as pl
from jax.experimental.pallas import tpu as pltpu
from jax.sharding import PartitionSpec as P

MESH = pl.DeviceIdType.MESH
HIGHEST = lax.Precision.HIGHEST
K = 40
STEPS = 3
SLOTS = 2
TPR = 8
LANES = 128
ROWS = 48
NEW = 44
FOLD = 16


def iota(shape, dim):
    return lax.broadcasted_iota(jnp.int32, shape, dim)


def far_first(step, count):
    half = lax.div(step + 1, 2)
    return count // 2 + half * (1 - 2 * lax.rem(step, 2))


def landed(ref, pieces, sem):
    view = ref.at[pl.ds(0, pieces)]
    pltpu.make_async_copy(view, view, sem).wait()


def sweep(matrix, rows, lanes, count):
    for k in range(count):
        column = matrix[:, k : k + 1]
        pivot = 1.0 / matrix[k : k + 1, k : k + 1]
        row = jnp.where(lanes[:1] == k, 1.0, matrix[k : k + 1, :]) * pivot
        cleared = jnp.where(lanes == k, 0.0, matrix) - column * row
        matrix = jnp.where(rows == k, row, cleared)
    return matrix


def kernel(
    n_dom, n_z, n_sub,
    load_hbm, recycled_hbm, images_hbm, tiles_hbm, columns_ref, ghosts_ref, live_ref,
    solution_ref, residual_ref,
    source, recycled, images, tiles, stack, gram, halo,
    sub_wide, x_wide, z_wide, sub_thin, x_thin, z_thin,
    load_sem, wide_send, wide_recv, thin_send, thin_recv, halo_send, halo_recv,
):
    n_x = n_dom // n_z
    dom, sub = lax.axis_index("dom"), lax.axis_index("sub")
    x, z = lax.div(dom, n_z), lax.rem(dom, n_z)
    group = n_sub * SLOTS
    own = group + sub * SLOTS

    loads = [
        pltpu.make_async_copy(src, dst, load_sem.at[i])
        for i, (src, dst) in enumerate(
            [(images_hbm, images), (load_hbm, source), (tiles_hbm, tiles), (recycled_hbm, recycled)]
        )
    ]
    for load in loads:
        load.start()

    def sub_peer(step):
        return lax.rem(sub + far_first(step, n_sub), n_sub)

    def x_peer(step):
        return lax.rem(x + far_first(step, n_x), n_x) * n_z + z

    def z_peer(step):
        return x * n_z + lax.rem(z + far_first(step, n_z), n_z)

    def each(count, body):
        def wrapped(step, carry):
            body(step)
            return carry

        lax.fori_loop(0, count, wrapped, 0)

    barrier = pltpu.get_barrier_semaphore()

    def greet(device):
        pl.semaphore_signal(barrier, inc=1, device_id=device, device_id_type=MESH)

    before, after = lax.rem(dom + n_dom - 1, n_dom), lax.rem(dom + 1, n_dom)
    each(n_sub, lambda j: greet((before, sub_peer(j))))
    each(n_sub, lambda j: greet((after, sub_peer(j))))
    each(n_sub - 1, lambda j: greet((dom, sub_peer(j))))
    each(n_x - 1, lambda j: greet((x_peer(j), sub)))
    each(n_z - 1, lambda j: greet((z_peer(j), sub)))

    masks = [jnp.where(live_ref[0] > s, 1.0, 0.0) for s in range(SLOTS)]

    stack[...] = jnp.zeros_like(stack)
    loads[0].wait()
    loads[1].wait()
    for s in range(SLOTS):
        stack[s, 0:K, :] = images[:, s, :] * masks[s]
        stack[s, K : K + 1, :] = source[s : s + 1, :] * masks[s]
    packed = jnp.zeros((FOLD, LANES), jnp.float32)
    for part in range(3):
        rows_of = slice(14 * part, 14 * part + FOLD)
        block = sum(
            lax.dot_general(
                stack[s, rows_of, :], stack[s], (((1,), (1,)), ((), ())),
                precision=HIGHEST, preferred_element_type=jnp.float32,
            )
            for s in range(SLOTS)
        )
        packed = packed + (pltpu.roll(block, 41 * part, 1) if part else block)

    pl.semaphore_wait(barrier, 3 * n_sub - 1 + n_x - 1 + n_z - 1)

    def spread(buffer, place, count, peer, send, recv):
        mine = buffer.at[place]
        each(
            count - 1,
            lambda j: pltpu.make_async_remote_copy(
                src_ref=mine, dst_ref=mine, send_sem=send, recv_sem=recv,
                device_id=peer(j), device_id_type=MESH,
            ).start(),
        )
        landed(buffer, count - 1, recv)

    def summed(value, sub_buf, x_buf, z_buf, send, recv):
        sub_buf[sub] = value
        spread(sub_buf, sub, n_sub, lambda j: (dom, sub_peer(j)), send.at[0], recv.at[0])
        x_buf[x] = jnp.sum(sub_buf[...], axis=0)
        spread(x_buf, x, n_x, lambda j: (x_peer(j), sub), send.at[1], recv.at[1])
        z_buf[z] = jnp.sum(x_buf[...], axis=0)
        spread(z_buf, z, n_z, lambda j: (z_peer(j), sub), send.at[2], recv.at[2])
        return jnp.sum(z_buf[...], axis=0)

    rows, lanes = iota((ROWS, LANES), 0), iota((ROWS, LANES), 1)
    row_of = iota((ROWS, 1), 0)

    total = summed(packed, sub_wide, x_wide, z_wide, wide_send, wide_recv)
    for part in range(3):
        piece = pltpu.roll(total, LANES - 41 * part, 1) if part else total
        gram[14 * part : 14 * part + FOLD, :] = piece
    start = jnp.where((lanes <= K) & (rows <= K), gram[...], 0.0)
    swept = sweep(start, rows, lanes, K)
    unit = jnp.where(rows == lanes, 1.0, 0.0)
    inverse = jnp.where((rows < K) & (lanes < K), swept, jnp.where(rows < K, 0.0, unit))
    start_coef = jnp.where(row_of < K, swept[:, K : K + 1], 0.0)
    initial_norm = jnp.sqrt(swept[K : K + 1, K : K + 1])

    def combined(s, coef):
        return jnp.sum(stack[s, 0:ROWS, :] * coef, axis=0, keepdims=True)

    residuals = [stack[s, K : K + 1, :] - combined(s, start_coef) for s in range(SLOTS)]
    basis = [[r / initial_norm for r in residuals]]

    places = []
    for s in range(SLOTS):
        for t in range(TPR):
            column = columns_ref[s, t]
            ghost = ghosts_ref[0, jnp.clip(column - SLOTS, 0, 3)]
            places.append(jnp.where(column < SLOTS, own + column, ghost))

    def exchange(blocks, r):
        here = halo.at[r]
        for s in range(SLOTS):
            here[own + s] = blocks[s]
        mine = here.at[pl.ds(own, SLOTS)]

        def send(shift, device):
            there = here.at[pl.ds((1 - shift) * group + sub * SLOTS, SLOTS)]
            pltpu.make_async_remote_copy(
                src_ref=mine, dst_ref=there, send_sem=halo_send.at[r], recv_sem=halo_recv.at[r],
                device_id=device, device_id_type=MESH,
            ).start()

        def far(j):
            send(-1, (before, sub_peer(j)))
            send(1, (after, sub_peer(j)))

        each(n_sub, far)
        each(n_sub - 1, lambda j: send(0, (dom, sub_peer(j))))
        landed(here, 3 * group - SLOTS, halo_recv.at[r])

    def multiply(r):
        images_now = []
        for s in range(SLOTS):
            grid = jnp.zeros((LANES, LANES), jnp.float32)
            for t in range(TPR):
                grid = grid + tiles[s, t] * halo[r, places[s * TPR + t]]
            images_now.append(jnp.sum(grid.T, axis=0, keepdims=True) * masks[s])
        return images_now

    loads[2].wait()
    coefs, products, norms = [], [], []
    for step in range(STEPS):
        for s in range(SLOTS):
            stack[s, K + step : K + step + 1, :] = basis[step][s]
        exchange(basis[step], step)
        image = multiply(step)
        for s in range(SLOTS):
            stack[s, NEW : NEW + 1, :] = image[s]
        grid = sum(stack[s] * image[s] for s in range(SLOTS))
        dots = jnp.sum(grid.T, axis=0, keepdims=True)
        dots = summed(
            dots, sub_thin.at[step], x_thin.at[step], z_thin.at[step],
            thin_send.at[step], thin_recv.at[step],
        )
        coef = jnp.sum(inverse * dots, axis=1, keepdims=True)
        product = jnp.sum(unit * dots, axis=1, keepdims=True)
        square = jnp.sum(
            jnp.where(row_of < NEW, -coef * product, jnp.where(row_of == NEW, product, 0.0)),
            axis=0, keepdims=True,
        )
        coef = jnp.where(row_of < NEW, coef, 0.0)
        norm = jnp.sqrt(square)
        basis.append([(image[s] - combined(s, coef)) / norm for s in range(SLOTS)])
        coefs.append(jnp.where(row_of < K, coef, 0.0))
        products.append(product)
        norms.append(norm)

    hess = [[None] * STEPS for _ in range(STEPS + 1)]
    for j in range(STEPS):
        for i in range(j + 1):
            hess[i][j] = products[j][K + i : K + i + 1, :]
        hess[j + 1][j] = norms[j]
    normal = [
        [sum(hess[i][a] * hess[i][b] for i in range(min(a, b) + 2)) for b in range(STEPS)]
        for a in range(STEPS)
    ]
    right = [initial_norm * hess[0][j] for j in range(STEPS)]
    for k in range(STEPS):
        for i in range(k + 1, STEPS):
            ratio = normal[k][i] / normal[k][k]
            for j in range(i, STEPS):
                normal[i][j] = normal[i][j] - ratio * normal[k][j]
            right[i] = right[i] - ratio * right[k]
    least = [None] * STEPS
    for k in reversed(range(STEPS)):
        rest = right[k]
        for j in range(k + 1, STEPS):
            rest = rest - normal[k][j] * least[j]
        least[k] = rest / normal[k][k]
    weights = [
        sum(hess[i][j] * least[j] for j in range(max(i - 1, 0), STEPS)) for i in range(STEPS + 1)
    ]

    update = start_coef - sum(least[j] * coefs[j] for j in range(STEPS))
    loads[3].wait()
    for s in range(SLOTS):
        from_recycled = jnp.sum(recycled[:, s, :] * update[0:K], axis=0, keepdims=True) * masks[s]
        solution_ref[s : s + 1, :] = from_recycled + sum(
            least[j] * basis[j][s] for j in range(STEPS)
        )
        residual_ref[s : s + 1, :] = residuals[s] - sum(
            weights[i] * basis[i][s] for i in range(STEPS + 1)
        )

    landed(sub_wide, n_sub - 1, wide_send.at[0])
    landed(x_wide, n_x - 1, wide_send.at[1])
    landed(z_wide, n_z - 1, wide_send.at[2])
    for step in range(STEPS):
        landed(sub_thin.at[step], n_sub - 1, thin_send.at[step, 0])
        landed(x_thin.at[step], n_x - 1, thin_send.at[step, 1])
        landed(z_thin.at[step], n_z - 1, thin_send.at[step, 2])
        landed(halo.at[step], 3 * group - SLOTS, halo_send.at[step])


def build(mesh, n_z):
    n_dom, n_sub = mesh.shape["dom"], mesh.shape["sub"]
    n_x = n_dom // n_z
    f32 = jnp.float32

    def local(load_vector, recycled, images, matrix_tiles, tile_columns, ghost_list, live_counts):
        anywhere = pl.BlockSpec(memory_space=pl.ANY)
        scalars = pl.BlockSpec(memory_space=pltpu.SMEM)
        vectors = pl.BlockSpec(memory_space=pltpu.VMEM)
        shape = jax.ShapeDtypeStruct(load_vector.shape, f32)
        dma = pltpu.SemaphoreType.DMA
        return pl.pallas_call(
            functools.partial(kernel, n_dom, n_z, n_sub),
            out_shape=(shape, shape),
            in_specs=[anywhere] * 4 + [scalars] * 3,
            out_specs=(vectors, vectors),
            scratch_shapes=[
                pltpu.VMEM(load_vector.shape, f32),
                pltpu.VMEM(recycled.shape, f32),
                pltpu.VMEM(images.shape, f32),
                pltpu.VMEM(matrix_tiles.shape, f32),
                pltpu.VMEM((SLOTS, LANES, LANES), f32),
                pltpu.VMEM((ROWS, LANES), f32),
                pltpu.VMEM((STEPS, 3 * n_sub * SLOTS, 1, LANES), f32),
                pltpu.VMEM((n_sub, FOLD, LANES), f32),
                pltpu.VMEM((n_x, FOLD, LANES), f32),
                pltpu.VMEM((n_z, FOLD, LANES), f32),
                pltpu.VMEM((STEPS, n_sub, 1, LANES), f32),
                pltpu.VMEM((STEPS, n_x, 1, LANES), f32),
                pltpu.VMEM((STEPS, n_z, 1, LANES), f32),
                dma((4,)),
                dma((3,)), dma((3,)),
                dma((STEPS, 3)), dma((STEPS, 3)),
                dma((STEPS,)), dma((STEPS,)),
            ],
            compiler_params=pltpu.CompilerParams(collective_id=0, has_side_effects=True),
        )(load_vector, recycled, images, matrix_tiles, tile_columns, ghost_list, live_counts)

    both = ("dom", "sub")
    in_specs = (
        P(both, None),
        P(None, both, None),
        P(None, both, None),
        P(both, None, None, None),
        P(both, None),
        P(both, None),
        P(both),
    )
    out_specs = (P(both, None), P(both, None))
    return jax.shard_map(local, mesh=mesh, in_specs=in_specs, out_specs=out_specs, check_vma=False)


def solution(mesh):
    return build(mesh, 8)
```

```python
import functools

import jax
import jax.numpy as jnp
from jax import lax
from jax.experimental import pallas as pl
from jax.experimental.pallas import tpu as pltpu
from jax.sharding import PartitionSpec as P

MESH = pl.DeviceIdType.MESH
HIGHEST = lax.Precision.HIGHEST
K = 40
STEPS = 3
SLOTS = 2
TPR = 8
GHOSTS = 4
BLOCKS = SLOTS + GHOSTS
CORES = 2
LANES = 128
ROWS = 48
NEW = 44
FOLD = 16


def iota(shape, dim):
    return lax.broadcasted_iota(jnp.int32, shape, dim)


def far_first(step, count):
    half = lax.div(step + 1, 2)
    return count // 2 + half * (1 - 2 * lax.rem(step, 2))


def landed(ref, pieces, sem):
    view = ref.at[pl.ds(0, pieces)]
    pltpu.make_async_copy(view, view, sem).wait()


def sweep(matrix, rows, lanes, count):
    for k in range(count):
        column = matrix[:, k : k + 1]
        pivot = 1.0 / matrix[k : k + 1, k : k + 1]
        row = jnp.where(lanes[:1] == k, 1.0, matrix[k : k + 1, :]) * pivot
        cleared = jnp.where(lanes == k, 0.0, matrix) - column * row
        matrix = jnp.where(rows == k, row, cleared)
    return matrix


def kernel(
    n_dom, n_z, n_sub,
    load_hbm, recycled_hbm, images_hbm, tiles_hbm, columns_ref, ghosts_ref, live_ref,
    solution_ref, residual_ref,
    source, recycled, images, tiles, stack, ghost_stack, gram, vectors, *more,
):
    halos, more = more[: STEPS - 1], more[STEPS - 1 :]
    line, asks, ask, asked, answers, answered, *more = more
    sub_wide, x_wide, z_wide, sub_thin, x_thin, z_thin, load_sem, *more = more
    wide_send, wide_recv, thin_send, thin_recv, halo_send, halo_recv, near_send, near_recv = more
    n_x = n_dom // n_z
    n_y = n_sub // CORES
    dom, sub = lax.axis_index("dom"), lax.axis_index("sub")
    x, z = lax.div(dom, n_z), lax.rem(dom, n_z)
    y, core = lax.div(sub, CORES), lax.rem(sub, CORES)
    group = n_sub * SLOTS
    own = group + sub * SLOTS

    loads = [
        pltpu.make_async_copy(src, dst, load_sem.at[i])
        for i, (src, dst) in enumerate(
            [(images_hbm, images), (load_hbm, source), (tiles_hbm, tiles), (recycled_hbm, recycled)]
        )
    ]
    for load in loads:
        load.start()

    def sub_peer(step):
        return lax.rem(sub + far_first(step, n_sub), n_sub)

    def y_peer(step):
        return lax.rem(y + far_first(step, n_y), n_y) * CORES + core

    def x_peer(step):
        return lax.rem(x + far_first(step, n_x), n_x) * n_z + z

    def z_peer(step):
        return x * n_z + lax.rem(z + far_first(step, n_z), n_z)

    def each(count, body):
        def wrapped(step, carry):
            body(step)
            return carry

        lax.fori_loop(0, count, wrapped, 0)

    barrier = pltpu.get_barrier_semaphore()

    def greet(device):
        pl.semaphore_signal(barrier, inc=1, device_id=device, device_id_type=MESH)

    before, after = lax.rem(dom + n_dom - 1, n_dom), lax.rem(dom + 1, n_dom)
    each(n_sub, lambda j: greet((before, sub_peer(j))))
    each(n_sub, lambda j: greet((after, sub_peer(j))))
    each(n_sub - 1, lambda j: greet((dom, sub_peer(j))))
    each(n_x - 1, lambda j: greet((x_peer(j), sub)))
    each(n_z - 1, lambda j: greet((z_peer(j), sub)))

    masks = [jnp.where(live_ref[0] > s, 1.0, 0.0) for s in range(SLOTS)]
    rows, lanes = iota((ROWS, LANES), 0), iota((ROWS, LANES), 1)
    row_of = iota((ROWS, 1), 0)

    ghost_codes = [ghosts_ref[0, g] for g in range(GHOSTS)]
    request = jnp.zeros((1, LANES), jnp.int32)
    for g in range(GHOSTS):
        request = jnp.where(lanes[:1] == g, ghost_codes[g], request)
    ask[0] = request
    asks[CORES + core] = request
    stack[...] = jnp.zeros_like(stack)
    loads[0].wait()
    loads[1].wait()
    for s in range(SLOTS):
        stack[s, 0:K, :] = images[:, s, :] * masks[s]
        stack[s, K : K + 1, :] = source[s : s + 1, :] * masks[s]
        line[y, s] = stack[s, 0:ROWS, :]
    packed = jnp.zeros((FOLD, LANES), jnp.float32)
    for part in range(3):
        rows_of = slice(14 * part, 14 * part + FOLD)
        block = sum(
            lax.dot_general(
                stack[s, rows_of, :], stack[s], (((1,), (1,)), ((), ())),
                precision=HIGHEST, preferred_element_type=jnp.float32,
            )
            for s in range(SLOTS)
        )
        packed = packed + (pltpu.roll(block, 41 * part, 1) if part else block)

    pl.semaphore_wait(barrier, 3 * n_sub - 1 + n_x - 1 + n_z - 1)

    def push(src, dst, send, recv, device):
        pltpu.make_async_remote_copy(
            src_ref=src, dst_ref=dst, send_sem=send, recv_sem=recv,
            device_id=device, device_id_type=MESH,
        ).start()

    def spread(buffer, place, count, peer, send, recv):
        mine = buffer.at[place]
        each(count - 1, lambda j: push(mine, mine, send, recv, peer(j)))

    near = [
        (shift, other)
        for shift in (-1, 1, 0)
        for other in ((0, 1) if shift else (1,))
    ]
    dom_at = {-1: before, 0: dom, 1: after}

    def core_at(other):
        return 1 - core if other else core

    sub_wide[sub] = packed
    spread(sub_wide, sub, n_sub, lambda j: (dom, sub_peer(j)), wide_send.at[0], wide_recv.at[0])
    for shift, other in near:
        device = (dom_at[shift], y * CORES + core_at(other))
        place = (1 - shift) * CORES + core
        push(ask.at[0], asks.at[place], near_send.at[0], near_recv.at[0], device)
    spread(line, y, n_y, lambda j: (dom, y_peer(j)), near_send.at[1], near_recv.at[1])
    landed(sub_wide, n_sub - 1, wide_recv.at[0])
    z_wide[z] = jnp.sum(sub_wide[...], axis=0)
    spread(z_wide, z, n_z, lambda j: (z_peer(j), sub), wide_send.at[1], wide_recv.at[1])
    landed(asks, len(near), near_recv.at[0])
    listed = pltpu.make_async_copy(asks, asked, load_sem.at[4])
    listed.start()
    listed.wait()
    landed(z_wide, n_z - 1, wide_recv.at[1])
    x_wide[x] = jnp.sum(z_wide[...], axis=0)
    spread(x_wide, x, n_x, lambda j: (x_peer(j), sub), wide_send.at[2], wide_recv.at[2])
    landed(line, n_y - 1, near_recv.at[1])

    def place_of(code):
        rest = lax.rem(code, group)
        return lax.div(rest, CORES * SLOTS), lax.rem(rest, SLOTS)

    for i, (shift, other) in enumerate(near):
        asker = (1 + shift) * CORES + core_at(other)
        for g in range(GHOSTS):
            answers[i, g] = line[place_of(asked[asker, 0, g])]
        device = (dom_at[shift], y * CORES + core_at(other))
        place = (1 - shift) * CORES + core
        push(answers.at[i], answered.at[place], near_send.at[2], near_recv.at[2], device)
    for g in range(GHOSTS):
        answered[CORES + core, g] = line[place_of(ghost_codes[g])]
    landed(x_wide, n_x - 1, wide_recv.at[2])
    total = jnp.sum(x_wide[...], axis=0)

    for part in range(3):
        piece = pltpu.roll(total, LANES - 41 * part, 1) if part else total
        gram[14 * part : 14 * part + FOLD, :] = piece
    start = jnp.where((lanes <= K) & (rows <= K), gram[...], 0.0)
    swept = sweep(start, rows, lanes, K)
    unit = jnp.where(rows == lanes, 1.0, 0.0)
    inverse = jnp.where((rows < K) & (lanes < K), swept, jnp.where(rows < K, 0.0, unit))
    start_coef = jnp.where(row_of < K, swept[:, K : K + 1], 0.0)
    initial_norm = jnp.sqrt(swept[K : K + 1, K : K + 1])

    landed(answered, len(near), near_recv.at[2])
    for g in range(GHOSTS):
        code = ghost_codes[g]
        held = lax.div(code, group) * CORES + lax.rem(lax.div(code, SLOTS), CORES)
        ghost_stack[g] = answered[held, g]

    def block(e):
        return stack[e, 0:ROWS, :] if e < SLOTS else ghost_stack[e - SLOTS]

    def combined(e, coef):
        return jnp.sum(block(e) * coef, axis=0, keepdims=True)

    def put(vector, step):
        for e, part in enumerate(vector):
            row = slice(K + step, K + step + 1)
            if e < SLOTS:
                stack[e, row, :] = part
            else:
                ghost_stack[e - SLOTS, row, :] = part
            vectors[step, e] = part

    residuals = [block(e)[K : K + 1, :] - combined(e, start_coef) for e in range(BLOCKS)]
    basis = [[r / initial_norm for r in residuals]]

    def send_halo(blocks, r):
        here = halos[r]
        for s in range(SLOTS):
            here[own + s] = blocks[s]
        mine = here.at[pl.ds(own, SLOTS)]

        def to(shift, device):
            there = here.at[pl.ds((1 - shift) * group + sub * SLOTS, SLOTS)]
            push(mine, there, halo_send.at[r], halo_recv.at[r], device)

        def far(j):
            to(-1, (before, sub_peer(j)))
            to(1, (after, sub_peer(j)))

        each(n_sub, far)
        each(n_sub - 1, lambda j: to(0, (dom, sub_peer(j))))

    def multiply(step):
        image = []
        for s in range(SLOTS):
            grid = jnp.zeros((LANES, LANES), jnp.float32)
            for t in range(TPR):
                grid = grid + tiles[s, t] * vectors[step, columns_ref[s, t]]
            image.append(jnp.sum(grid.T, axis=0, keepdims=True) * masks[s])
        return image

    loads[2].wait()
    coefs, products, norms = [], [], []
    for step in range(STEPS):
        last = step == STEPS - 1
        put(basis[step], step)
        image = multiply(step)
        for s in range(SLOTS):
            stack[s, NEW : NEW + 1, :] = image[s]
        grid = sum(stack[s] * image[s] for s in range(SLOTS))
        across, down, along = sub_thin.at[step], z_thin.at[step], x_thin.at[step]
        send, recv = thin_send.at[step], thin_recv.at[step]
        across[sub] = jnp.sum(grid.T, axis=0, keepdims=True)
        spread(across, sub, n_sub, lambda j: (dom, sub_peer(j)), send.at[0], recv.at[0])
        if not last:
            send_halo(image, step)
        landed(across, n_sub - 1, recv.at[0])
        down[z] = jnp.sum(across[...], axis=0)
        spread(down, z, n_z, lambda j: (z_peer(j), sub), send.at[1], recv.at[1])
        landed(down, n_z - 1, recv.at[1])
        along[x] = jnp.sum(down[...], axis=0)
        spread(along, x, n_x, lambda j: (x_peer(j), sub), send.at[2], recv.at[2])
        landed(along, n_x - 1, recv.at[2])
        dots = jnp.sum(along[...], axis=0)
        coef = jnp.sum(inverse * dots, axis=1, keepdims=True)
        product = jnp.sum(unit * dots, axis=1, keepdims=True)
        square = jnp.sum(
            jnp.where(row_of < NEW, -coef * product, jnp.where(row_of == NEW, product, 0.0)),
            axis=0, keepdims=True,
        )
        coef = jnp.where(row_of < NEW, coef, 0.0)
        norm = jnp.sqrt(square)
        if not last:
            landed(halos[step], 3 * group - SLOTS, halo_recv.at[step])
            image = image + [halos[step][ghost_codes[g]] for g in range(GHOSTS)]
        basis.append([(part - combined(e, coef)) / norm for e, part in enumerate(image)])
        coefs.append(jnp.where(row_of < K, coef, 0.0))
        products.append(product)
        norms.append(norm)

    hess = [[None] * STEPS for _ in range(STEPS + 1)]
    for j in range(STEPS):
        for i in range(j + 1):
            hess[i][j] = products[j][K + i : K + i + 1, :]
        hess[j + 1][j] = norms[j]
    normal = [
        [sum(hess[i][a] * hess[i][b] for i in range(min(a, b) + 2)) for b in range(STEPS)]
        for a in range(STEPS)
    ]
    right = [initial_norm * hess[0][j] for j in range(STEPS)]
    for k in range(STEPS):
        for i in range(k + 1, STEPS):
            ratio = normal[k][i] / normal[k][k]
            for j in range(i, STEPS):
                normal[i][j] = normal[i][j] - ratio * normal[k][j]
            right[i] = right[i] - ratio * right[k]
    least = [None] * STEPS
    for k in reversed(range(STEPS)):
        rest = right[k]
        for j in range(k + 1, STEPS):
            rest = rest - normal[k][j] * least[j]
        least[k] = rest / normal[k][k]
    weights = [
        sum(hess[i][j] * least[j] for j in range(max(i - 1, 0), STEPS)) for i in range(STEPS + 1)
    ]

    update = start_coef - sum(least[j] * coefs[j] for j in range(STEPS))
    loads[3].wait()
    for s in range(SLOTS):
        from_recycled = jnp.sum(recycled[:, s, :] * update[0:K], axis=0, keepdims=True) * masks[s]
        solution_ref[s : s + 1, :] = from_recycled + sum(
            least[j] * basis[j][s] for j in range(STEPS)
        )
        residual_ref[s : s + 1, :] = residuals[s] - sum(
            weights[i] * basis[i][s] for i in range(STEPS + 1)
        )

    landed(sub_wide, n_sub - 1, wide_send.at[0])
    landed(z_wide, n_z - 1, wide_send.at[1])
    landed(x_wide, n_x - 1, wide_send.at[2])
    landed(asks, len(near), near_send.at[0])
    landed(line, n_y - 1, near_send.at[1])
    landed(answers, len(near), near_send.at[2])
    for step in range(STEPS):
        landed(sub_thin.at[step], n_sub - 1, thin_send.at[step, 0])
        landed(z_thin.at[step], n_z - 1, thin_send.at[step, 1])
        landed(x_thin.at[step], n_x - 1, thin_send.at[step, 2])
        if step < STEPS - 1:
            landed(halos[step], 3 * group - SLOTS, halo_send.at[step])


def build(mesh, n_z):
    n_dom, n_sub = mesh.shape["dom"], mesh.shape["sub"]
    n_x, n_y = n_dom // n_z, n_sub // CORES
    f32 = jnp.float32

    def local(load_vector, recycled, images, matrix_tiles, tile_columns, ghost_list, live_counts):
        anywhere = pl.BlockSpec(memory_space=pl.ANY)
        scalars = pl.BlockSpec(memory_space=pltpu.SMEM)
        vectors = pl.BlockSpec(memory_space=pltpu.VMEM)
        shape = jax.ShapeDtypeStruct(load_vector.shape, f32)
        dma = pltpu.SemaphoreType.DMA
        asks = (3 * CORES, 1, LANES)
        return pl.pallas_call(
            functools.partial(kernel, n_dom, n_z, n_sub),
            out_shape=(shape, shape),
            in_specs=[anywhere] * 4 + [scalars] * 3,
            out_specs=(vectors, vectors),
            scratch_shapes=[
                pltpu.VMEM(load_vector.shape, f32),
                pltpu.VMEM(recycled.shape, f32),
                pltpu.VMEM(images.shape, f32),
                pltpu.VMEM(matrix_tiles.shape, f32),
                pltpu.VMEM((SLOTS, LANES, LANES), f32),
                pltpu.VMEM((GHOSTS, ROWS, LANES), f32),
                pltpu.VMEM((ROWS, LANES), f32),
                pltpu.VMEM((STEPS, BLOCKS, 1, LANES), f32),
                *[pltpu.VMEM((3 * n_sub * SLOTS, 1, LANES), f32)] * (STEPS - 1),
                pltpu.VMEM((n_y, SLOTS, ROWS, LANES), f32),
                pltpu.VMEM(asks, jnp.int32),
                pltpu.VMEM((1, 1, LANES), jnp.int32),
                pltpu.SMEM(asks, jnp.int32),
                pltpu.VMEM((3 * CORES - 1, GHOSTS, ROWS, LANES), f32),
                pltpu.VMEM((3 * CORES, GHOSTS, ROWS, LANES), f32),
                pltpu.VMEM((n_sub, FOLD, LANES), f32),
                pltpu.VMEM((n_x, FOLD, LANES), f32),
                pltpu.VMEM((n_z, FOLD, LANES), f32),
                pltpu.VMEM((STEPS, n_sub, 1, LANES), f32),
                pltpu.VMEM((STEPS, n_x, 1, LANES), f32),
                pltpu.VMEM((STEPS, n_z, 1, LANES), f32),
                dma((5,)),
                dma((3,)), dma((3,)),
                dma((STEPS, 3)), dma((STEPS, 3)),
                dma((STEPS - 1,)), dma((STEPS - 1,)),
                dma((3,)), dma((3,)),
            ],
            compiler_params=pltpu.CompilerParams(collective_id=0, has_side_effects=True),
        )(load_vector, recycled, images, matrix_tiles, tile_columns, ghost_list, live_counts)

    both = ("dom", "sub")
    in_specs = (
        P(both, None),
        P(None, both, None),
        P(None, both, None),
        P(both, None, None, None),
        P(both, None),
        P(both, None),
        P(both),
    )
    out_specs = (P(both, None), P(both, None))
    return jax.shard_map(local, mesh=mesh, in_specs=in_specs, out_specs=out_specs, check_vma=False)


def solution(mesh):
    return build(mesh, 8)
```

```python
import functools

import jax
import jax.numpy as jnp
from jax import lax
from jax.experimental import pallas as pl
from jax.experimental.pallas import tpu as pltpu
from jax.sharding import PartitionSpec as P

MESH = pl.DeviceIdType.MESH
HIGHEST = lax.Precision.HIGHEST
K = 40
STEPS = 3
SLOTS = 2
TPR = 8
GHOSTS = 4
BLOCKS = SLOTS + GHOSTS
CORES = 2
PIVOTS = 4
LANES = 128
ROWS = 48
NEW = 44
FOLD = 16


def iota(shape, dim):
    return lax.broadcasted_iota(jnp.int32, shape, dim)


def far_first(step, count):
    half = lax.div(step + 1, 2)
    return count // 2 + half * (1 - 2 * lax.rem(step, 2))


def landed(ref, pieces, sem):
    view = ref.at[pl.ds(0, pieces)]
    pltpu.make_async_copy(view, view, sem).wait()


def sweep(matrix, rows, lanes, count):
    for first in range(0, count, PIVOTS):
        steps = range(first, first + PIVOTS)
        columns = [jnp.broadcast_to(matrix[:, k : k + 1], matrix.shape) for k in steps]
        for i, k in enumerate(steps):
            column = columns[i]
            pivot = 1.0 / column[k : k + 1, :]
            row = jnp.where(lanes[:1] == k, 1.0, matrix[k : k + 1, :]) * pivot
            cleared = jnp.where(lanes == k, 0.0, matrix) - column * row
            matrix = jnp.where(rows == k, row, cleared)
            for j in range(i + 1, PIVOTS):
                scale = columns[j][k : k + 1, :] * pivot
                columns[j] = jnp.where(rows == k, scale, columns[j] - column * scale)
    return matrix


def kernel(
    n_dom, n_z, n_sub,
    load_hbm, recycled_hbm, images_hbm, tiles_hbm, columns_ref, ghosts_ref, live_ref,
    parts_ref,
    source, recycled, images, tiles, stack, ghost_stack, gram, vectors, *more,
):
    halos, more = more[: STEPS - 1], more[STEPS - 1 :]
    line, asks, ask, asked, answers, answered, *more = more
    sub_wide, x_wide, z_wide, sub_thin, x_thin, z_thin, load_sem, *more = more
    wide_send, wide_recv, thin_send, thin_recv, halo_send, halo_recv, near_send, near_recv, hop_recv = more
    n_x = n_dom // n_z
    n_y = n_sub // CORES
    dom, sub = lax.axis_index("dom"), lax.axis_index("sub")
    x, z = lax.div(dom, n_z), lax.rem(dom, n_z)
    y, core = lax.div(sub, CORES), lax.rem(sub, CORES)
    group = n_sub * SLOTS
    own = group + sub * SLOTS

    loads = [
        pltpu.make_async_copy(src, dst, load_sem.at[i])
        for i, (src, dst) in enumerate(
            [(images_hbm, images), (load_hbm, source), (tiles_hbm, tiles), (recycled_hbm, recycled)]
        )
    ]
    for load in loads:
        load.start()

    def sub_peer(step):
        return lax.rem(sub + far_first(step, n_sub), n_sub)

    def x_peer(step):
        return lax.rem(x + far_first(step, n_x), n_x) * n_z + z

    def z_peer(step):
        return x * n_z + lax.rem(z + far_first(step, n_z), n_z)

    def each(count, body):
        def wrapped(step, carry):
            body(step)
            return carry

        lax.fori_loop(0, count, wrapped, 0)

    barrier = pltpu.get_barrier_semaphore()

    def greet(device):
        pl.semaphore_signal(barrier, inc=1, device_id=device, device_id_type=MESH)

    before, after = lax.rem(dom + n_dom - 1, n_dom), lax.rem(dom + 1, n_dom)
    each(n_sub, lambda j: greet((before, sub_peer(j))))
    each(n_sub, lambda j: greet((after, sub_peer(j))))
    each(n_sub - 1, lambda j: greet((dom, sub_peer(j))))
    each(n_x - 1, lambda j: greet((x_peer(j), sub)))
    each(n_z - 1, lambda j: greet((z_peer(j), sub)))

    masks = [jnp.where(live_ref[0] > s, 1.0, 0.0) for s in range(SLOTS)]
    rows, lanes = iota((ROWS, LANES), 0), iota((ROWS, LANES), 1)
    row_of = iota((ROWS, 1), 0)

    ghost_codes = [ghosts_ref[0, g] for g in range(GHOSTS)]
    request = jnp.zeros((1, LANES), jnp.int32)
    for g in range(GHOSTS):
        request = jnp.where(lanes[:1] == g, ghost_codes[g], request)
    ask[0] = request
    asks[CORES + core] = request
    stack[...] = jnp.zeros_like(stack)
    loads[0].wait()
    loads[1].wait()
    for s in range(SLOTS):
        stack[s, 0:K, :] = images[:, s, :] * masks[s]
        stack[s, K : K + 1, :] = source[s : s + 1, :] * masks[s]
        line[y, s] = stack[s, 0:ROWS, :]
    packed = jnp.zeros((FOLD, LANES), jnp.float32)
    for part in range(3):
        rows_of = slice(14 * part, 14 * part + FOLD)
        block = sum(
            lax.dot_general(
                stack[s, rows_of, :], stack[s], (((1,), (1,)), ((), ())),
                precision=HIGHEST, preferred_element_type=jnp.float32,
            )
            for s in range(SLOTS)
        )
        packed = packed + (pltpu.roll(block, 41 * part, 1) if part else block)

    pl.semaphore_wait(barrier, 3 * n_sub - 1 + n_x - 1 + n_z - 1)

    def push(src, dst, send, recv, device):
        pltpu.make_async_remote_copy(
            src_ref=src, dst_ref=dst, send_sem=send, recv_sem=recv,
            device_id=device, device_id_type=MESH,
        ).start()

    def spread(buffer, place, count, peer, send, recv):
        mine = buffer.at[place]
        each(count - 1, lambda j: push(mine, mine, send, recv, peer(j)))

    def along_y(piece, hops, send, recv):
        device = (dom, lax.rem(y + hops + n_y, n_y) * CORES + core)
        push(piece, piece, send, recv, device)

    near = [
        (shift, other)
        for shift in (-1, 1, 0)
        for other in ((0, 1) if shift else (1,))
    ]
    dom_at = {-1: before, 0: dom, 1: after}

    def core_at(other):
        return 1 - core if other else core

    sub_wide[sub] = packed
    spread(sub_wide, sub, n_sub, lambda j: (dom, sub_peer(j)), wide_send.at[0], wide_recv.at[0])
    for shift, other in near:
        device = (dom_at[shift], y * CORES + core_at(other))
        place = (1 - shift) * CORES + core
        push(ask.at[0], asks.at[place], near_send.at[0], near_recv.at[0], device)
    for i, hops in enumerate((2, -2, 1, -1)):
        along_y(line.at[y], hops, near_send.at[1], hop_recv.at[i])
    landed(sub_wide, n_sub - 1, wide_recv.at[0])
    z_wide[z] = jnp.sum(sub_wide[...], axis=0)
    spread(z_wide, z, n_z, lambda j: (z_peer(j), sub), wide_send.at[1], wide_recv.at[1])
    for i, sign in enumerate((1, -1)):
        landed(line, 1, hop_recv.at[i])
        held = line.at[lax.rem(y - 2 * sign + n_y, n_y)]
        along_y(held, sign, near_send.at[1], hop_recv.at[4 + i])
        along_y(held.at[pl.ds(i, 1)], 2 * sign, near_send.at[1], hop_recv.at[6 + i])
    landed(asks, len(near), near_recv.at[0])
    listed = pltpu.make_async_copy(asks, asked, load_sem.at[4])
    listed.start()
    listed.wait()
    landed(z_wide, n_z - 1, wide_recv.at[1])
    x_wide[x] = jnp.sum(z_wide[...], axis=0)
    spread(x_wide, x, n_x, lambda j: (x_peer(j), sub), wide_send.at[2], wide_recv.at[2])
    for i in range(2, 6):
        landed(line, 1, hop_recv.at[i])
    for i in range(6, 8):
        landed(line.at[0], 1, hop_recv.at[i])

    def place_of(code):
        rest = lax.rem(code, group)
        return lax.div(rest, CORES * SLOTS), lax.rem(rest, SLOTS)

    for i, (shift, other) in enumerate(near):
        asker = (1 + shift) * CORES + core_at(other)
        for g in range(GHOSTS):
            answers[i, g] = line[place_of(asked[asker, 0, g])]
        device = (dom_at[shift], y * CORES + core_at(other))
        place = (1 - shift) * CORES + core
        push(answers.at[i], answered.at[place], near_send.at[2], near_recv.at[2], device)
    for g in range(GHOSTS):
        answered[CORES + core, g] = line[place_of(ghost_codes[g])]
    landed(x_wide, n_x - 1, wide_recv.at[2])
    total = jnp.sum(x_wide[...], axis=0)

    for part in range(3):
        piece = pltpu.roll(total, LANES - 41 * part, 1) if part else total
        gram[14 * part : 14 * part + FOLD, :] = piece
    start = jnp.where((lanes <= K) & (rows <= K), gram[...], 0.0)
    swept = sweep(start, rows, lanes, K)
    unit = jnp.where(rows == lanes, 1.0, 0.0)
    inverse = jnp.where((rows < K) & (lanes < K), swept, jnp.where(rows < K, 0.0, unit))
    start_coef = jnp.where(row_of < K, swept[:, K : K + 1], 0.0)
    initial_norm = jnp.sqrt(swept[K : K + 1, K : K + 1])

    landed(answered, len(near), near_recv.at[2])
    for g in range(GHOSTS):
        code = ghost_codes[g]
        held = lax.div(code, group) * CORES + lax.rem(lax.div(code, SLOTS), CORES)
        ghost_stack[g] = answered[held, g]

    def block(e):
        return stack[e, 0:ROWS, :] if e < SLOTS else ghost_stack[e - SLOTS]

    def combined(e, coef):
        return jnp.sum(block(e) * coef, axis=0, keepdims=True)

    def put(vector, step):
        for e, part in enumerate(vector):
            row = slice(K + step, K + step + 1)
            if e < SLOTS:
                stack[e, row, :] = part
            else:
                ghost_stack[e - SLOTS, row, :] = part
            vectors[step, e] = part

    residuals = [block(e)[K : K + 1, :] - combined(e, start_coef) for e in range(BLOCKS)]
    basis = [[r / initial_norm for r in residuals]]

    def send_halo(blocks, r):
        here = halos[r]
        for s in range(SLOTS):
            here[own + s] = blocks[s]
        mine = here.at[pl.ds(own, SLOTS)]

        def to(shift, device):
            there = here.at[pl.ds((1 - shift) * group + sub * SLOTS, SLOTS)]
            push(mine, there, halo_send.at[r], halo_recv.at[r], device)

        def far(j):
            to(-1, (before, sub_peer(j)))
            to(1, (after, sub_peer(j)))

        each(n_sub, far)
        each(n_sub - 1, lambda j: to(0, (dom, sub_peer(j))))

    def multiply(step):
        image = []
        for s in range(SLOTS):
            grid = jnp.zeros((LANES, LANES), jnp.float32)
            for t in range(TPR):
                grid = grid + tiles[s, t] * vectors[step, columns_ref[s, t]]
            image.append(jnp.sum(grid.T, axis=0, keepdims=True) * masks[s])
        return image

    loads[2].wait()
    coefs, products, norms = [], [], []
    for step in range(STEPS):
        last = step == STEPS - 1
        put(basis[step], step)
        image = multiply(step)
        for s in range(SLOTS):
            stack[s, NEW : NEW + 1, :] = image[s]
        grid = sum(stack[s] * image[s] for s in range(SLOTS))
        across, down, along = sub_thin.at[step], z_thin.at[step], x_thin.at[step]
        send, recv = thin_send.at[step], thin_recv.at[step]
        across[sub] = jnp.sum(grid.T, axis=0, keepdims=True)
        spread(across, sub, n_sub, lambda j: (dom, sub_peer(j)), send.at[0], recv.at[0])
        if not last:
            send_halo(image, step)
        landed(across, n_sub - 1, recv.at[0])
        down[z] = jnp.sum(across[...], axis=0)
        spread(down, z, n_z, lambda j: (z_peer(j), sub), send.at[1], recv.at[1])
        landed(down, n_z - 1, recv.at[1])
        along[x] = jnp.sum(down[...], axis=0)
        spread(along, x, n_x, lambda j: (x_peer(j), sub), send.at[2], recv.at[2])
        landed(along, n_x - 1, recv.at[2])
        dots = jnp.sum(along[...], axis=0)
        coef = jnp.sum(inverse * dots, axis=1, keepdims=True)
        product = jnp.sum(unit * dots, axis=1, keepdims=True)
        square = jnp.sum(
            jnp.where(row_of < NEW, -coef * product, jnp.where(row_of == NEW, product, 0.0)),
            axis=0, keepdims=True,
        )
        coef = jnp.where(row_of < NEW, coef, 0.0)
        norm = jnp.sqrt(square)
        if not last:
            landed(halos[step], 3 * group - SLOTS, halo_recv.at[step])
            image = image + [halos[step][ghost_codes[g]] for g in range(GHOSTS)]
        basis.append([(part - combined(e, coef)) / norm for e, part in enumerate(image)])
        coefs.append(jnp.where(row_of < K, coef, 0.0))
        products.append(product)
        norms.append(norm)

    hess = [[None] * STEPS for _ in range(STEPS + 1)]
    for j in range(STEPS):
        for i in range(j + 1):
            hess[i][j] = products[j][K + i : K + i + 1, :]
        hess[j + 1][j] = norms[j]
    normal = [
        [sum(hess[i][a] * hess[i][b] for i in range(min(a, b) + 2)) for b in range(STEPS)]
        for a in range(STEPS)
    ]
    right = [initial_norm * hess[0][j] for j in range(STEPS)]
    for k in range(STEPS):
        for i in range(k + 1, STEPS):
            ratio = normal[k][i] / normal[k][k]
            for j in range(i, STEPS):
                normal[i][j] = normal[i][j] - ratio * normal[k][j]
            right[i] = right[i] - ratio * right[k]
    least = [None] * STEPS
    for k in reversed(range(STEPS)):
        rest = right[k]
        for j in range(k + 1, STEPS):
            rest = rest - normal[k][j] * least[j]
        least[k] = rest / normal[k][k]
    weights = [
        sum(hess[i][j] * least[j] for j in range(max(i - 1, 0), STEPS)) for i in range(STEPS + 1)
    ]

    update = start_coef - sum(least[j] * coefs[j] for j in range(STEPS))
    loads[3].wait()
    for s in range(SLOTS):
        from_recycled = jnp.sum(recycled[:, s, :] * update[0:K], axis=0, keepdims=True) * masks[s]
        parts_ref[0, s : s + 1, :] = from_recycled
        parts_ref[1, s : s + 1, :] = sum(least[j] * basis[j][s] for j in range(STEPS))
        parts_ref[2, s : s + 1, :] = residuals[s]
        parts_ref[3, s : s + 1, :] = sum(weights[i] * basis[i][s] for i in range(STEPS + 1))

    landed(sub_wide, n_sub - 1, wide_send.at[0])
    landed(z_wide, n_z - 1, wide_send.at[1])
    landed(x_wide, n_x - 1, wide_send.at[2])
    landed(asks, len(near), near_send.at[0])
    landed(line, n_y - 1, near_send.at[1])
    landed(answers, len(near), near_send.at[2])
    for step in range(STEPS):
        landed(sub_thin.at[step], n_sub - 1, thin_send.at[step, 0])
        landed(z_thin.at[step], n_z - 1, thin_send.at[step, 1])
        landed(x_thin.at[step], n_x - 1, thin_send.at[step, 2])
        if step < STEPS - 1:
            landed(halos[step], 3 * group - SLOTS, halo_send.at[step])


def build(mesh, n_z):
    n_dom, n_sub = mesh.shape["dom"], mesh.shape["sub"]
    n_x, n_y = n_dom // n_z, n_sub // CORES
    f32 = jnp.float32

    def local(load_vector, recycled, images, matrix_tiles, tile_columns, ghost_list, live_counts):
        anywhere = pl.BlockSpec(memory_space=pl.ANY)
        scalars = pl.BlockSpec(memory_space=pltpu.SMEM)
        vectors = pl.BlockSpec(memory_space=pltpu.VMEM)
        dma = pltpu.SemaphoreType.DMA
        asks = (3 * CORES, 1, LANES)
        parts = pl.pallas_call(
            functools.partial(kernel, n_dom, n_z, n_sub),
            out_shape=jax.ShapeDtypeStruct((4, *load_vector.shape), f32),
            in_specs=[anywhere] * 4 + [scalars] * 3,
            out_specs=vectors,
            scratch_shapes=[
                pltpu.VMEM(load_vector.shape, f32),
                pltpu.VMEM(recycled.shape, f32),
                pltpu.VMEM(images.shape, f32),
                pltpu.VMEM(matrix_tiles.shape, f32),
                pltpu.VMEM((SLOTS, LANES, LANES), f32),
                pltpu.VMEM((GHOSTS, ROWS, LANES), f32),
                pltpu.VMEM((ROWS, LANES), f32),
                pltpu.VMEM((STEPS, BLOCKS, 1, LANES), f32),
                *[pltpu.VMEM((3 * n_sub * SLOTS, 1, LANES), f32)] * (STEPS - 1),
                pltpu.VMEM((n_y, SLOTS, ROWS, LANES), f32),
                pltpu.VMEM(asks, jnp.int32),
                pltpu.VMEM((1, 1, LANES), jnp.int32),
                pltpu.SMEM(asks, jnp.int32),
                pltpu.VMEM((3 * CORES - 1, GHOSTS, ROWS, LANES), f32),
                pltpu.VMEM((3 * CORES, GHOSTS, ROWS, LANES), f32),
                pltpu.VMEM((n_sub, FOLD, LANES), f32),
                pltpu.VMEM((n_x, FOLD, LANES), f32),
                pltpu.VMEM((n_z, FOLD, LANES), f32),
                pltpu.VMEM((STEPS, n_sub, 1, LANES), f32),
                pltpu.VMEM((STEPS, n_x, 1, LANES), f32),
                pltpu.VMEM((STEPS, n_z, 1, LANES), f32),
                dma((5,)),
                dma((3,)), dma((3,)),
                dma((STEPS, 3)), dma((STEPS, 3)),
                dma((STEPS - 1,)), dma((STEPS - 1,)),
                dma((3,)), dma((3,)), dma((8,)),
            ],
            compiler_params=pltpu.CompilerParams(collective_id=0, has_side_effects=True),
        )(load_vector, recycled, images, matrix_tiles, tile_columns, ghost_list, live_counts)
        return parts[0] + parts[1], parts[2] - parts[3]

    both = ("dom", "sub")
    in_specs = (
        P(both, None),
        P(None, both, None),
        P(None, both, None),
        P(both, None, None, None),
        P(both, None),
        P(both, None),
        P(both),
    )
    out_specs = (P(both, None), P(both, None))
    return jax.shard_map(local, mesh=mesh, in_specs=in_specs, out_specs=out_specs, check_vma=False)


def solution(mesh):
    return build(mesh, 8)
```

```python
import functools

import jax
import jax.numpy as jnp
from jax import lax
from jax.experimental import pallas as pl
from jax.experimental.pallas import tpu as pltpu
from jax.sharding import PartitionSpec as P

MESH = pl.DeviceIdType.MESH
HIGHEST = lax.Precision.HIGHEST
K = 40
STEPS = 3
SLOTS = 2
TPR = 8
GHOSTS = 4
BLOCKS = SLOTS + GHOSTS
CORES = 2
PIVOTS = 4
LANES = 128
ROWS = 48
NEW = 44
FOLD = 16


def iota(shape, dim):
    return lax.broadcasted_iota(jnp.int32, shape, dim)


def far_first(step, count):
    half = lax.div(step + 1, 2)
    return count // 2 + half * (1 - 2 * lax.rem(step, 2))


def landed(ref, pieces, sem):
    view = ref.at[pl.ds(0, pieces)]
    pltpu.make_async_copy(view, view, sem).wait()


def sweep(matrix, rows, lanes, count):
    for first in range(0, count, PIVOTS):
        steps = range(first, first + PIVOTS)
        columns = [jnp.broadcast_to(matrix[:, k : k + 1], matrix.shape) for k in steps]
        for i, k in enumerate(steps):
            column = columns[i]
            pivot = 1.0 / column[k : k + 1, :]
            row = jnp.where(lanes[:1] == k, 1.0, matrix[k : k + 1, :]) * pivot
            cleared = jnp.where(lanes == k, 0.0, matrix) - column * row
            matrix = jnp.where(rows == k, row, cleared)
            for j in range(i + 1, PIVOTS):
                scale = columns[j][k : k + 1, :] * pivot
                columns[j] = jnp.where(rows == k, scale, columns[j] - column * scale)
    return matrix


def kernel(
    n_dom, n_z, n_sub,
    load_hbm, recycled_hbm, images_hbm, tiles_hbm, columns_ref, ghosts_ref, live_ref,
    parts_ref,
    source, recycled, images, tiles, stack, ghost_stack, gram, vectors, *more,
):
    halos, more = more[: STEPS - 1], more[STEPS - 1 :]
    line, asks, ask, asked, answers, answered, *more = more
    sub_wide, x_wide, z_wide, sub_thin, plane_thin, load_sem, *more = more
    wide_send, wide_recv, thin_send, thin_recv, halo_send, halo_recv, near_send, near_recv, hop_recv = more
    n_x = n_dom // n_z
    n_y = n_sub // CORES
    dom, sub = lax.axis_index("dom"), lax.axis_index("sub")
    x, z = lax.div(dom, n_z), lax.rem(dom, n_z)
    y, core = lax.div(sub, CORES), lax.rem(sub, CORES)
    group = n_sub * SLOTS
    own = group + sub * SLOTS

    loads = [
        pltpu.make_async_copy(src, dst, load_sem.at[i])
        for i, (src, dst) in enumerate(
            [(images_hbm, images), (load_hbm, source), (tiles_hbm, tiles), (recycled_hbm, recycled)]
        )
    ]
    for load in loads:
        load.start()

    def sub_peer(step):
        return lax.rem(sub + far_first(step, n_sub), n_sub)

    def x_peer(step):
        return lax.rem(x + far_first(step, n_x), n_x) * n_z + z

    def z_peer(step):
        return x * n_z + lax.rem(z + far_first(step, n_z), n_z)

    def plane_peer(i, j):
        across = lax.rem(x + far_first(i, n_x), n_x)
        return across * n_z + lax.rem(z + far_first(j, n_z), n_z)

    def each(count, body):
        def wrapped(step, carry):
            body(step)
            return carry

        lax.fori_loop(0, count, wrapped, 0)

    def each_of_plane(body):
        each(n_x - 1, lambda i: each(n_z, lambda j: body(plane_peer(i, j))))
        each(n_z - 1, lambda j: body(plane_peer(n_x - 1, j)))

    barrier = pltpu.get_barrier_semaphore()

    def greet(device):
        pl.semaphore_signal(barrier, inc=1, device_id=device, device_id_type=MESH)

    before, after = lax.rem(dom + n_dom - 1, n_dom), lax.rem(dom + 1, n_dom)
    each(n_sub, lambda j: greet((before, sub_peer(j))))
    each(n_sub, lambda j: greet((after, sub_peer(j))))
    each(n_sub - 1, lambda j: greet((dom, sub_peer(j))))
    each_of_plane(lambda peer: greet((peer, sub)))

    masks = [jnp.where(live_ref[0] > s, 1.0, 0.0) for s in range(SLOTS)]
    rows, lanes = iota((ROWS, LANES), 0), iota((ROWS, LANES), 1)
    row_of = iota((ROWS, 1), 0)

    ghost_codes = [ghosts_ref[0, g] for g in range(GHOSTS)]
    request = jnp.zeros((1, LANES), jnp.int32)
    for g in range(GHOSTS):
        request = jnp.where(lanes[:1] == g, ghost_codes[g], request)
    ask[0] = request
    asks[CORES + core] = request
    stack[...] = jnp.zeros_like(stack)
    loads[0].wait()
    loads[1].wait()
    for s in range(SLOTS):
        stack[s, 0:K, :] = images[:, s, :] * masks[s]
        stack[s, K : K + 1, :] = source[s : s + 1, :] * masks[s]
        line[y, s] = stack[s, 0:ROWS, :]
    packed = jnp.zeros((FOLD, LANES), jnp.float32)
    for part in range(3):
        rows_of = slice(14 * part, 14 * part + FOLD)
        block = sum(
            lax.dot_general(
                stack[s, rows_of, :], stack[s], (((1,), (1,)), ((), ())),
                precision=HIGHEST, preferred_element_type=jnp.float32,
            )
            for s in range(SLOTS)
        )
        packed = packed + (pltpu.roll(block, 41 * part, 1) if part else block)

    pl.semaphore_wait(barrier, 3 * n_sub - 1 + n_dom - 1)

    def push(src, dst, send, recv, device):
        pltpu.make_async_remote_copy(
            src_ref=src, dst_ref=dst, send_sem=send, recv_sem=recv,
            device_id=device, device_id_type=MESH,
        ).start()

    def spread(buffer, place, count, peer, send, recv):
        mine = buffer.at[place]
        each(count - 1, lambda j: push(mine, mine, send, recv, peer(j)))

    def along_y(piece, hops, send, recv):
        device = (dom, lax.rem(y + hops + n_y, n_y) * CORES + core)
        push(piece, piece, send, recv, device)

    near = [
        (shift, other)
        for shift in (-1, 1, 0)
        for other in ((0, 1) if shift else (1,))
    ]
    dom_at = {-1: before, 0: dom, 1: after}

    def core_at(other):
        return 1 - core if other else core

    sub_wide[sub] = packed
    spread(sub_wide, sub, n_sub, lambda j: (dom, sub_peer(j)), wide_send.at[0], wide_recv.at[0])
    for shift, other in near:
        device = (dom_at[shift], y * CORES + core_at(other))
        place = (1 - shift) * CORES + core
        push(ask.at[0], asks.at[place], near_send.at[0], near_recv.at[0], device)
    for i, hops in enumerate((2, -2, 1, -1)):
        along_y(line.at[y], hops, near_send.at[1], hop_recv.at[i])
    landed(sub_wide, n_sub - 1, wide_recv.at[0])
    z_wide[z] = jnp.sum(sub_wide[...], axis=0)
    spread(z_wide, z, n_z, lambda j: (z_peer(j), sub), wide_send.at[1], wide_recv.at[1])
    for i, sign in enumerate((1, -1)):
        landed(line, 1, hop_recv.at[i])
        held = line.at[lax.rem(y - 2 * sign + n_y, n_y)]
        along_y(held, sign, near_send.at[1], hop_recv.at[4 + i])
        along_y(held.at[pl.ds(i, 1)], 2 * sign, near_send.at[1], hop_recv.at[6 + i])
    landed(asks, len(near), near_recv.at[0])
    listed = pltpu.make_async_copy(asks, asked, load_sem.at[4])
    listed.start()
    listed.wait()
    landed(z_wide, n_z - 1, wide_recv.at[1])
    x_wide[x] = jnp.sum(z_wide[...], axis=0)
    spread(x_wide, x, n_x, lambda j: (x_peer(j), sub), wide_send.at[2], wide_recv.at[2])
    for i in range(2, 6):
        landed(line, 1, hop_recv.at[i])
    for i in range(6, 8):
        landed(line.at[0], 1, hop_recv.at[i])

    def place_of(code):
        rest = lax.rem(code, group)
        return lax.div(rest, CORES * SLOTS), lax.rem(rest, SLOTS)

    for i, (shift, other) in enumerate(near):
        asker = (1 + shift) * CORES + core_at(other)
        for g in range(GHOSTS):
            answers[i, g] = line[place_of(asked[asker, 0, g])]
        device = (dom_at[shift], y * CORES + core_at(other))
        place = (1 - shift) * CORES + core
        push(answers.at[i], answered.at[place], near_send.at[2], near_recv.at[2], device)
    for g in range(GHOSTS):
        answered[CORES + core, g] = line[place_of(ghost_codes[g])]
    landed(x_wide, n_x - 1, wide_recv.at[2])
    total = jnp.sum(x_wide[...], axis=0)

    for part in range(3):
        piece = pltpu.roll(total, LANES - 41 * part, 1) if part else total
        gram[14 * part : 14 * part + FOLD, :] = piece
    start = jnp.where((lanes <= K) & (rows <= K), gram[...], 0.0)
    swept = sweep(start, rows, lanes, K)
    unit = jnp.where(rows == lanes, 1.0, 0.0)
    inverse = jnp.where((rows < K) & (lanes < K), swept, jnp.where(rows < K, 0.0, unit))
    start_coef = jnp.where(row_of < K, swept[:, K : K + 1], 0.0)
    initial_norm = jnp.sqrt(swept[K : K + 1, K : K + 1])

    landed(answered, len(near), near_recv.at[2])
    for g in range(GHOSTS):
        code = ghost_codes[g]
        held = lax.div(code, group) * CORES + lax.rem(lax.div(code, SLOTS), CORES)
        ghost_stack[g] = answered[held, g]

    def block(e):
        return stack[e, 0:ROWS, :] if e < SLOTS else ghost_stack[e - SLOTS]

    def combined(e, coef):
        return jnp.sum(block(e) * coef, axis=0, keepdims=True)

    def put(vector, step):
        for e, part in enumerate(vector):
            row = slice(K + step, K + step + 1)
            if e < SLOTS:
                stack[e, row, :] = part
            else:
                ghost_stack[e - SLOTS, row, :] = part
            vectors[step, e] = part

    residuals = [block(e)[K : K + 1, :] - combined(e, start_coef) for e in range(BLOCKS)]
    basis = [[r / initial_norm for r in residuals]]

    def send_halo(blocks, r):
        here = halos[r]
        for s in range(SLOTS):
            here[own + s] = blocks[s]
        mine = here.at[pl.ds(own, SLOTS)]

        def to(shift, device):
            there = here.at[pl.ds((1 - shift) * group + sub * SLOTS, SLOTS)]
            push(mine, there, halo_send.at[r], halo_recv.at[r], device)

        def far(j):
            to(-1, (before, sub_peer(j)))
            to(1, (after, sub_peer(j)))

        each(n_sub, far)
        each(n_sub - 1, lambda j: to(0, (dom, sub_peer(j))))

    def multiply(step):
        image = []
        for s in range(SLOTS):
            grid = jnp.zeros((LANES, LANES), jnp.float32)
            for t in range(TPR):
                grid = grid + tiles[s, t] * vectors[step, columns_ref[s, t]]
            image.append(jnp.sum(grid.T, axis=0, keepdims=True) * masks[s])
        return image

    loads[2].wait()
    coefs, products, norms = [], [], []
    for step in range(STEPS):
        last = step == STEPS - 1
        put(basis[step], step)
        image = multiply(step)
        for s in range(SLOTS):
            stack[s, NEW : NEW + 1, :] = image[s]
        grid = sum(stack[s] * image[s] for s in range(SLOTS))
        across, plane = sub_thin.at[step], plane_thin.at[step]
        send, recv = thin_send.at[step], thin_recv.at[step]
        across[sub] = jnp.sum(grid.T, axis=0, keepdims=True)
        spread(across, sub, n_sub, lambda j: (dom, sub_peer(j)), send.at[0], recv.at[0])
        if not last:
            send_halo(image, step)
        landed(across, n_sub - 1, recv.at[0])
        plane[dom] = jnp.sum(across[...], axis=0)
        mine = plane.at[dom]
        each_of_plane(lambda peer: push(mine, mine, send.at[1], recv.at[1], (peer, sub)))
        landed(plane, n_dom - 1, recv.at[1])
        dots = jnp.sum(plane[...], axis=0)
        coef = jnp.sum(inverse * dots, axis=1, keepdims=True)
        product = jnp.sum(unit * dots, axis=1, keepdims=True)
        square = jnp.sum(
            jnp.where(row_of < NEW, -coef * product, jnp.where(row_of == NEW, product, 0.0)),
            axis=0, keepdims=True,
        )
        coef = jnp.where(row_of < NEW, coef, 0.0)
        norm = jnp.sqrt(square)
        if not last:
            landed(halos[step], 3 * group - SLOTS, halo_recv.at[step])
            image = image + [halos[step][ghost_codes[g]] for g in range(GHOSTS)]
        basis.append([(part - combined(e, coef)) / norm for e, part in enumerate(image)])
        coefs.append(jnp.where(row_of < K, coef, 0.0))
        products.append(product)
        norms.append(norm)

    hess = [[None] * STEPS for _ in range(STEPS + 1)]
    for j in range(STEPS):
        for i in range(j + 1):
            hess[i][j] = products[j][K + i : K + i + 1, :]
        hess[j + 1][j] = norms[j]
    normal = [
        [sum(hess[i][a] * hess[i][b] for i in range(min(a, b) + 2)) for b in range(STEPS)]
        for a in range(STEPS)
    ]
    right = [initial_norm * hess[0][j] for j in range(STEPS)]
    for k in range(STEPS):
        for i in range(k + 1, STEPS):
            ratio = normal[k][i] / normal[k][k]
            for j in range(i, STEPS):
                normal[i][j] = normal[i][j] - ratio * normal[k][j]
            right[i] = right[i] - ratio * right[k]
    least = [None] * STEPS
    for k in reversed(range(STEPS)):
        rest = right[k]
        for j in range(k + 1, STEPS):
            rest = rest - normal[k][j] * least[j]
        least[k] = rest / normal[k][k]
    weights = [
        sum(hess[i][j] * least[j] for j in range(max(i - 1, 0), STEPS)) for i in range(STEPS + 1)
    ]

    update = start_coef - sum(least[j] * coefs[j] for j in range(STEPS))
    loads[3].wait()
    for s in range(SLOTS):
        from_recycled = jnp.sum(recycled[:, s, :] * update[0:K], axis=0, keepdims=True) * masks[s]
        parts_ref[0, s : s + 1, :] = from_recycled
        parts_ref[1, s : s + 1, :] = sum(least[j] * basis[j][s] for j in range(STEPS))
        parts_ref[2, s : s + 1, :] = residuals[s]
        parts_ref[3, s : s + 1, :] = sum(weights[i] * basis[i][s] for i in range(STEPS + 1))

    landed(sub_wide, n_sub - 1, wide_send.at[0])
    landed(z_wide, n_z - 1, wide_send.at[1])
    landed(x_wide, n_x - 1, wide_send.at[2])
    landed(asks, len(near), near_send.at[0])
    landed(line, n_y - 1, near_send.at[1])
    landed(answers, len(near), near_send.at[2])
    for step in range(STEPS):
        landed(sub_thin.at[step], n_sub - 1, thin_send.at[step, 0])
        landed(plane_thin.at[step], n_dom - 1, thin_send.at[step, 1])
        if step < STEPS - 1:
            landed(halos[step], 3 * group - SLOTS, halo_send.at[step])


def build(mesh, n_z):
    n_dom, n_sub = mesh.shape["dom"], mesh.shape["sub"]
    n_x, n_y = n_dom // n_z, n_sub // CORES
    f32 = jnp.float32

    def local(load_vector, recycled, images, matrix_tiles, tile_columns, ghost_list, live_counts):
        anywhere = pl.BlockSpec(memory_space=pl.ANY)
        scalars = pl.BlockSpec(memory_space=pltpu.SMEM)
        vectors = pl.BlockSpec(memory_space=pltpu.VMEM)
        dma = pltpu.SemaphoreType.DMA
        asks = (3 * CORES, 1, LANES)
        parts = pl.pallas_call(
            functools.partial(kernel, n_dom, n_z, n_sub),
            out_shape=jax.ShapeDtypeStruct((4, *load_vector.shape), f32),
            in_specs=[anywhere] * 4 + [scalars] * 3,
            out_specs=vectors,
            scratch_shapes=[
                pltpu.VMEM(load_vector.shape, f32),
                pltpu.VMEM(recycled.shape, f32),
                pltpu.VMEM(images.shape, f32),
                pltpu.VMEM(matrix_tiles.shape, f32),
                pltpu.VMEM((SLOTS, LANES, LANES), f32),
                pltpu.VMEM((GHOSTS, ROWS, LANES), f32),
                pltpu.VMEM((ROWS, LANES), f32),
                pltpu.VMEM((STEPS, BLOCKS, 1, LANES), f32),
                *[pltpu.VMEM((3 * n_sub * SLOTS, 1, LANES), f32)] * (STEPS - 1),
                pltpu.VMEM((n_y, SLOTS, ROWS, LANES), f32),
                pltpu.VMEM(asks, jnp.int32),
                pltpu.VMEM((1, 1, LANES), jnp.int32),
                pltpu.SMEM(asks, jnp.int32),
                pltpu.VMEM((3 * CORES - 1, GHOSTS, ROWS, LANES), f32),
                pltpu.VMEM((3 * CORES, GHOSTS, ROWS, LANES), f32),
                pltpu.VMEM((n_sub, FOLD, LANES), f32),
                pltpu.VMEM((n_x, FOLD, LANES), f32),
                pltpu.VMEM((n_z, FOLD, LANES), f32),
                pltpu.VMEM((STEPS, n_sub, 1, LANES), f32),
                pltpu.VMEM((STEPS, n_dom, 1, LANES), f32),
                dma((5,)),
                dma((3,)), dma((3,)),
                dma((STEPS, 2)), dma((STEPS, 2)),
                dma((STEPS - 1,)), dma((STEPS - 1,)),
                dma((3,)), dma((3,)), dma((8,)),
            ],
            compiler_params=pltpu.CompilerParams(collective_id=0, has_side_effects=True),
        )(load_vector, recycled, images, matrix_tiles, tile_columns, ghost_list, live_counts)
        return parts[0] + parts[1], parts[2] - parts[3]

    both = ("dom", "sub")
    in_specs = (
        P(both, None),
        P(None, both, None),
        P(None, both, None),
        P(both, None, None, None),
        P(both, None),
        P(both, None),
        P(both),
    )
    out_specs = (P(both, None), P(both, None))
    return jax.shard_map(local, mesh=mesh, in_specs=in_specs, out_specs=out_specs, check_vma=False)


def solution(mesh):
    return build(mesh, 8)
```

```python
import functools

import jax
import jax.numpy as jnp
from jax import lax
from jax.experimental import pallas as pl
from jax.experimental.pallas import tpu as pltpu
from jax.sharding import PartitionSpec as P

MESH = pl.DeviceIdType.MESH
HIGHEST = lax.Precision.HIGHEST
K = 40
STEPS = 3
SLOTS = 2
TPR = 8
GHOSTS = 4
BLOCKS = SLOTS + GHOSTS
CORES = 2
PIVOTS = 4
LANES = 128
ROWS = 48
NEW = 44
FOLD = 16


def iota(shape, dim):
    return lax.broadcasted_iota(jnp.int32, shape, dim)


def far_first(step, count):
    half = lax.div(step + 1, 2)
    return count // 2 + half * (1 - 2 * lax.rem(step, 2))


def landed(ref, pieces, sem):
    view = ref.at[pl.ds(0, pieces)]
    pltpu.make_async_copy(view, view, sem).wait()


def sweep(matrix, rows, lanes, count):
    for first in range(0, count, PIVOTS):
        steps = range(first, first + PIVOTS)
        columns = [jnp.broadcast_to(matrix[:, k : k + 1], matrix.shape) for k in steps]
        for i, k in enumerate(steps):
            column = columns[i]
            pivot = 1.0 / column[k : k + 1, :]
            row = jnp.where(lanes[:1] == k, 1.0, matrix[k : k + 1, :]) * pivot
            cleared = jnp.where(lanes == k, 0.0, matrix) - column * row
            matrix = jnp.where(rows == k, row, cleared)
            for j in range(i + 1, PIVOTS):
                scale = columns[j][k : k + 1, :] * pivot
                columns[j] = jnp.where(rows == k, scale, columns[j] - column * scale)
    return matrix


def kernel(
    n_dom, n_z, n_sub,
    load_hbm, recycled_hbm, images_hbm, tiles_hbm, columns_hbm, ghosts_hbm, live_ref,
    parts_ref,
    columns_ref, ghosts_ref, source, recycled, images, tiles, stack, ghost_stack, gram, vectors, *more,
):
    halos, more = more[: STEPS - 1], more[STEPS - 1 :]
    line, asks, ask, asked, answers, answered, *more = more
    sub_wide, x_wide, z_wide, sub_thin, plane_thin, load_sem, *more = more
    wide_send, wide_recv, thin_send, thin_recv, halo_send, halo_recv, near_send, near_recv, hop_recv = more
    n_x = n_dom // n_z
    n_y = n_sub // CORES
    dom, sub = lax.axis_index("dom"), lax.axis_index("sub")
    x, z = lax.div(dom, n_z), lax.rem(dom, n_z)
    y, core = lax.div(sub, CORES), lax.rem(sub, CORES)
    group = n_sub * SLOTS
    own = group + sub * SLOTS

    loads = [
        pltpu.make_async_copy(src, dst, load_sem.at[i])
        for i, (src, dst) in enumerate(
            [(images_hbm, images), (load_hbm, source), (tiles_hbm, tiles), (recycled_hbm, recycled)]
        )
    ]
    listings = [
        pltpu.make_async_copy(ghosts_hbm, ghosts_ref, load_sem.at[5]),
        pltpu.make_async_copy(columns_hbm, columns_ref, load_sem.at[6]),
    ]
    for load in loads + listings:
        load.start()

    def sub_peer(step):
        return lax.rem(sub + far_first(step, n_sub), n_sub)

    def x_peer(step):
        return lax.rem(x + far_first(step, n_x), n_x) * n_z + z

    def z_peer(step):
        return x * n_z + lax.rem(z + far_first(step, n_z), n_z)

    def plane_peer(i, j):
        across = lax.rem(x + far_first(i, n_x), n_x)
        return across * n_z + lax.rem(z + far_first(j, n_z), n_z)

    def each(count, body):
        def wrapped(step, carry):
            body(step)
            return carry

        lax.fori_loop(0, count, wrapped, 0)

    def each_of_plane(body):
        each(n_x - 1, lambda i: each(n_z, lambda j: body(plane_peer(i, j))))
        each(n_z - 1, lambda j: body(plane_peer(n_x - 1, j)))

    barrier = pltpu.get_barrier_semaphore()

    def greet(device):
        pl.semaphore_signal(barrier, inc=1, device_id=device, device_id_type=MESH)

    before, after = lax.rem(dom + n_dom - 1, n_dom), lax.rem(dom + 1, n_dom)
    each_of_plane(lambda peer: greet((peer, sub)))
    each(n_sub, lambda j: greet((before, sub_peer(j))))
    each(n_sub, lambda j: greet((after, sub_peer(j))))
    each(n_sub - 1, lambda j: greet((dom, sub_peer(j))))

    for listing in listings:
        listing.wait()
    masks = [jnp.where(live_ref[0] > s, 1.0, 0.0) for s in range(SLOTS)]
    rows, lanes = iota((ROWS, LANES), 0), iota((ROWS, LANES), 1)
    row_of = iota((ROWS, 1), 0)

    ghost_codes = [ghosts_ref[0, g] for g in range(GHOSTS)]
    request = jnp.zeros((1, LANES), jnp.int32)
    for g in range(GHOSTS):
        request = jnp.where(lanes[:1] == g, ghost_codes[g], request)
    ask[0] = request
    asks[CORES + core] = request
    stack[...] = jnp.zeros_like(stack)
    loads[0].wait()
    loads[1].wait()
    for s in range(SLOTS):
        stack[s, 0:K, :] = images[:, s, :] * masks[s]
        stack[s, K : K + 1, :] = source[s : s + 1, :] * masks[s]
        line[y, s] = stack[s, 0:ROWS, :]
    packed = jnp.zeros((FOLD, LANES), jnp.float32)
    for part in range(3):
        rows_of = slice(14 * part, 14 * part + FOLD)
        block = sum(
            lax.dot_general(
                stack[s, rows_of, :], stack[s], (((1,), (1,)), ((), ())),
                precision=HIGHEST, preferred_element_type=jnp.float32,
            )
            for s in range(SLOTS)
        )
        packed = packed + (pltpu.roll(block, 41 * part, 1) if part else block)

    pl.semaphore_wait(barrier, 3 * n_sub - 1 + n_dom - 1)

    def push(src, dst, send, recv, device):
        pltpu.make_async_remote_copy(
            src_ref=src, dst_ref=dst, send_sem=send, recv_sem=recv,
            device_id=device, device_id_type=MESH,
        ).start()

    def spread(buffer, place, count, peer, send, recv):
        mine = buffer.at[place]
        each(count - 1, lambda j: push(mine, mine, send, recv, peer(j)))

    def along_y(piece, hops, send, recv):
        device = (dom, lax.rem(y + hops + n_y, n_y) * CORES + core)
        push(piece, piece, send, recv, device)

    near = [
        (shift, other)
        for shift in (-1, 1, 0)
        for other in ((0, 1) if shift else (1,))
    ]
    dom_at = {-1: before, 0: dom, 1: after}

    def core_at(other):
        return 1 - core if other else core

    sub_wide[sub] = packed
    spread(sub_wide, sub, n_sub, lambda j: (dom, sub_peer(j)), wide_send.at[0], wide_recv.at[0])
    for shift, other in near:
        device = (dom_at[shift], y * CORES + core_at(other))
        place = (1 - shift) * CORES + core
        push(ask.at[0], asks.at[place], near_send.at[0], near_recv.at[0], device)
    for i, hops in enumerate((2, -2, 1, -1)):
        along_y(line.at[y], hops, near_send.at[1], hop_recv.at[i])
    landed(sub_wide, n_sub - 1, wide_recv.at[0])
    z_wide[z] = jnp.sum(sub_wide[...], axis=0)
    spread(z_wide, z, n_z, lambda j: (z_peer(j), sub), wide_send.at[1], wide_recv.at[1])
    for i, sign in enumerate((1, -1)):
        landed(line, 1, hop_recv.at[i])
        held = line.at[lax.rem(y - 2 * sign + n_y, n_y)]
        along_y(held, sign, near_send.at[1], hop_recv.at[4 + i])
        along_y(held.at[pl.ds(i, 1)], 2 * sign, near_send.at[1], hop_recv.at[6 + i])
    landed(asks, len(near), near_recv.at[0])
    listed = pltpu.make_async_copy(asks, asked, load_sem.at[4])
    listed.start()
    listed.wait()
    landed(z_wide, n_z - 1, wide_recv.at[1])
    x_wide[x] = jnp.sum(z_wide[...], axis=0)
    spread(x_wide, x, n_x, lambda j: (x_peer(j), sub), wide_send.at[2], wide_recv.at[2])
    for i in range(2, 6):
        landed(line, 1, hop_recv.at[i])
    for i in range(6, 8):
        landed(line.at[0], 1, hop_recv.at[i])

    def place_of(code):
        rest = lax.rem(code, group)
        return lax.div(rest, CORES * SLOTS), lax.rem(rest, SLOTS)

    for i, (shift, other) in enumerate(near):
        asker = (1 + shift) * CORES + core_at(other)
        for g in range(GHOSTS):
            answers[i, g] = line[place_of(asked[asker, 0, g])]
        device = (dom_at[shift], y * CORES + core_at(other))
        place = (1 - shift) * CORES + core
        push(answers.at[i], answered.at[place], near_send.at[2], near_recv.at[2], device)
    for g in range(GHOSTS):
        answered[CORES + core, g] = line[place_of(ghost_codes[g])]
    landed(x_wide, n_x - 1, wide_recv.at[2])
    total = jnp.sum(x_wide[...], axis=0)

    for part in range(3):
        piece = pltpu.roll(total, LANES - 41 * part, 1) if part else total
        gram[14 * part : 14 * part + FOLD, :] = piece
    start = jnp.where((lanes <= K) & (rows <= K), gram[...], 0.0)
    swept = sweep(start, rows, lanes, K)
    unit = jnp.where(rows == lanes, 1.0, 0.0)
    inverse = jnp.where((rows < K) & (lanes < K), swept, jnp.where(rows < K, 0.0, unit))
    start_coef = jnp.where(row_of < K, swept[:, K : K + 1], 0.0)
    initial_norm = jnp.sqrt(swept[K : K + 1, K : K + 1])

    landed(answered, len(near), near_recv.at[2])
    for g in range(GHOSTS):
        code = ghost_codes[g]
        held = lax.div(code, group) * CORES + lax.rem(lax.div(code, SLOTS), CORES)
        ghost_stack[g] = answered[held, g]

    def block(e):
        return stack[e, 0:ROWS, :] if e < SLOTS else ghost_stack[e - SLOTS]

    def combined(e, coef):
        return jnp.sum(block(e) * coef, axis=0, keepdims=True)

    def put(vector, step):
        for e, part in enumerate(vector):
            row = slice(K + step, K + step + 1)
            if e < SLOTS:
                stack[e, row, :] = part
            else:
                ghost_stack[e - SLOTS, row, :] = part
            vectors[step, e] = part

    residuals = [block(e)[K : K + 1, :] - combined(e, start_coef) for e in range(BLOCKS)]
    basis = [[r / initial_norm for r in residuals]]

    def send_halo(blocks, r):
        here = halos[r]
        for s in range(SLOTS):
            here[own + s] = blocks[s]
        mine = here.at[pl.ds(own, SLOTS)]

        def to(shift, device):
            there = here.at[pl.ds((1 - shift) * group + sub * SLOTS, SLOTS)]
            push(mine, there, halo_send.at[r], halo_recv.at[r], device)

        def far(j):
            to(-1, (before, sub_peer(j)))
            to(1, (after, sub_peer(j)))

        each(n_sub, far)
        each(n_sub - 1, lambda j: to(0, (dom, sub_peer(j))))

    def multiply(step):
        image = []
        for s in range(SLOTS):
            grid = jnp.zeros((LANES, LANES), jnp.float32)
            for t in range(TPR):
                grid = grid + tiles[s, t] * vectors[step, columns_ref[s, t]]
            image.append(jnp.sum(grid.T, axis=0, keepdims=True) * masks[s])
        return image

    loads[2].wait()
    coefs, products, norms = [], [], []
    for step in range(STEPS):
        last = step == STEPS - 1
        put(basis[step], step)
        image = multiply(step)
        for s in range(SLOTS):
            stack[s, NEW : NEW + 1, :] = image[s]
        grid = sum(stack[s] * image[s] for s in range(SLOTS))
        across, plane = sub_thin.at[step], plane_thin.at[step]
        send, recv = thin_send.at[step], thin_recv.at[step]
        across[sub] = jnp.sum(grid.T, axis=0, keepdims=True)
        spread(across, sub, n_sub, lambda j: (dom, sub_peer(j)), send.at[0], recv.at[0])
        if not last:
            send_halo(image, step)
        landed(across, n_sub - 1, recv.at[0])
        plane[dom] = jnp.sum(across[...], axis=0)
        mine = plane.at[dom]
        each_of_plane(lambda peer: push(mine, mine, send.at[1], recv.at[1], (peer, sub)))
        landed(plane, n_dom - 1, recv.at[1])
        dots = jnp.sum(plane[...], axis=0)
        coef = jnp.sum(inverse * dots, axis=1, keepdims=True)
        product = jnp.sum(unit * dots, axis=1, keepdims=True)
        square = jnp.sum(
            jnp.where(row_of < NEW, -coef * product, jnp.where(row_of == NEW, product, 0.0)),
            axis=0, keepdims=True,
        )
        coef = jnp.where(row_of < NEW, coef, 0.0)
        norm = jnp.sqrt(square)
        if not last:
            landed(halos[step], 3 * group - SLOTS, halo_recv.at[step])
            image = image + [halos[step][ghost_codes[g]] for g in range(GHOSTS)]
        basis.append([(part - combined(e, coef)) / norm for e, part in enumerate(image)])
        coefs.append(jnp.where(row_of < K, coef, 0.0))
        products.append(product)
        norms.append(norm)

    hess = [[None] * STEPS for _ in range(STEPS + 1)]
    for j in range(STEPS):
        for i in range(j + 1):
            hess[i][j] = products[j][K + i : K + i + 1, :]
        hess[j + 1][j] = norms[j]
    normal = [
        [sum(hess[i][a] * hess[i][b] for i in range(min(a, b) + 2)) for b in range(STEPS)]
        for a in range(STEPS)
    ]
    right = [initial_norm * hess[0][j] for j in range(STEPS)]
    for k in range(STEPS):
        for i in range(k + 1, STEPS):
            ratio = normal[k][i] / normal[k][k]
            for j in range(i, STEPS):
                normal[i][j] = normal[i][j] - ratio * normal[k][j]
            right[i] = right[i] - ratio * right[k]
    least = [None] * STEPS
    for k in reversed(range(STEPS)):
        rest = right[k]
        for j in range(k + 1, STEPS):
            rest = rest - normal[k][j] * least[j]
        least[k] = rest / normal[k][k]
    weights = [
        sum(hess[i][j] * least[j] for j in range(max(i - 1, 0), STEPS)) for i in range(STEPS + 1)
    ]

    update = start_coef - sum(least[j] * coefs[j] for j in range(STEPS))
    loads[3].wait()
    for s in range(SLOTS):
        from_recycled = jnp.sum(recycled[:, s, :] * update[0:K], axis=0, keepdims=True) * masks[s]
        parts_ref[0, s : s + 1, :] = from_recycled
        parts_ref[1, s : s + 1, :] = sum(least[j] * basis[j][s] for j in range(STEPS))
        parts_ref[2, s : s + 1, :] = residuals[s]
        parts_ref[3, s : s + 1, :] = sum(weights[i] * basis[i][s] for i in range(STEPS + 1))

    landed(sub_wide, n_sub - 1, wide_send.at[0])
    landed(z_wide, n_z - 1, wide_send.at[1])
    landed(x_wide, n_x - 1, wide_send.at[2])
    landed(asks, len(near), near_send.at[0])
    landed(line, n_y - 1, near_send.at[1])
    landed(answers, len(near), near_send.at[2])
    for step in range(STEPS):
        landed(sub_thin.at[step], n_sub - 1, thin_send.at[step, 0])
        landed(plane_thin.at[step], n_dom - 1, thin_send.at[step, 1])
        if step < STEPS - 1:
            landed(halos[step], 3 * group - SLOTS, halo_send.at[step])


def build(mesh, n_z):
    n_dom, n_sub = mesh.shape["dom"], mesh.shape["sub"]
    n_x, n_y = n_dom // n_z, n_sub // CORES
    f32 = jnp.float32

    def local(load_vector, recycled, images, matrix_tiles, tile_columns, ghost_list, live_counts):
        anywhere = pl.BlockSpec(memory_space=pl.ANY)
        scalars = pl.BlockSpec(memory_space=pltpu.SMEM)
        vectors = pl.BlockSpec(memory_space=pltpu.VMEM)
        dma = pltpu.SemaphoreType.DMA
        asks = (3 * CORES, 1, LANES)
        parts = pl.pallas_call(
            functools.partial(kernel, n_dom, n_z, n_sub),
            out_shape=jax.ShapeDtypeStruct((4, *load_vector.shape), f32),
            in_specs=[anywhere] * 6 + [scalars],
            out_specs=vectors,
            scratch_shapes=[
                pltpu.SMEM(tile_columns.shape, jnp.int32),
                pltpu.SMEM(ghost_list.shape, jnp.int32),
                pltpu.VMEM(load_vector.shape, f32),
                pltpu.VMEM(recycled.shape, f32),
                pltpu.VMEM(images.shape, f32),
                pltpu.VMEM(matrix_tiles.shape, f32),
                pltpu.VMEM((SLOTS, LANES, LANES), f32),
                pltpu.VMEM((GHOSTS, ROWS, LANES), f32),
                pltpu.VMEM((ROWS, LANES), f32),
                pltpu.VMEM((STEPS, BLOCKS, 1, LANES), f32),
                *[pltpu.VMEM((3 * n_sub * SLOTS, 1, LANES), f32)] * (STEPS - 1),
                pltpu.VMEM((n_y, SLOTS, ROWS, LANES), f32),
                pltpu.VMEM(asks, jnp.int32),
                pltpu.VMEM((1, 1, LANES), jnp.int32),
                pltpu.SMEM(asks, jnp.int32),
                pltpu.VMEM((3 * CORES - 1, GHOSTS, ROWS, LANES), f32),
                pltpu.VMEM((3 * CORES, GHOSTS, ROWS, LANES), f32),
                pltpu.VMEM((n_sub, FOLD, LANES), f32),
                pltpu.VMEM((n_x, FOLD, LANES), f32),
                pltpu.VMEM((n_z, FOLD, LANES), f32),
                pltpu.VMEM((STEPS, n_sub, 1, LANES), f32),
                pltpu.VMEM((STEPS, n_dom, 1, LANES), f32),
                dma((7,)),
                dma((3,)), dma((3,)),
                dma((STEPS, 2)), dma((STEPS, 2)),
                dma((STEPS - 1,)), dma((STEPS - 1,)),
                dma((3,)), dma((3,)), dma((8,)),
            ],
            compiler_params=pltpu.CompilerParams(collective_id=0, has_side_effects=True),
        )(load_vector, recycled, images, matrix_tiles, tile_columns, ghost_list, live_counts)
        return parts[0] + parts[1], parts[2] - parts[3]

    both = ("dom", "sub")
    in_specs = (
        P(both, None),
        P(None, both, None),
        P(None, both, None),
        P(both, None, None, None),
        P(both, None),
        P(both, None),
        P(both),
    )
    out_specs = (P(both, None), P(both, None))
    return jax.shard_map(local, mesh=mesh, in_specs=in_specs, out_specs=out_specs, check_vma=False)


def solution(mesh):
    return build(mesh, 8)
```
